512 devices in a mesh: band: 16 (over z), ga: 32 (over y, x, core).
Axes of the slice: x: 4, y: 4, z: 16, core: 2. Of those that a mesh axis runs over, the one named last changes fastest.
Arguments:
- waves: bfloat16 [2, 512, 32768], P(None, 'band', 'ga'), may hold values from -6 to 6
- occupations: float32 [512], P('band'), may hold values from 0.000390625 to 0.0078125
- beta_table: float32 [72, 32768], P(None, 'ga'), may hold values from -0.0234375 to 0.0234375
- wave_miller: int32 [3, 32768], P(None, 'ga'), may hold values from 0 to 223
- atom_kinds: int32 [256], replicated, may hold values from 0 to 3
- atom_sites: int32 [3, 256], replicated, may hold values from 0 to 223
- aug_table: bfloat16 [684, 917504], P(None, ('band', 'ga')), may hold values from -0.00015258789 to 0.00015258789
- stick_columns: int32 [4096], P(('band', 'ga')), may hold values from -1 to 3599, as said below
Outputs:
- density: float32 [2, 224, 240, 240], P(None, 'ga', 'band')
The draws below stay inside these ranges and needn't reach their ends.
Inputs may be any that keep to these rules, and one draw needn't show every extreme that they name: `stick_columns`: entry t is a slot of the device at place t // 8 in band-major order, of band index t // 256. -1 marks an empty slot; otherwise the entry c names the column x = (t // 256) * 15 + c // 240, y = c mod 240. Live columns of one band index are distinct. On each device the live slots come first and at least one is live; in each band index some device has all 8 slots live.
All inputs are finite; a program needn't handle non-finite values.
Results may differ from the reference program's by a relative error of at most 0.0035.
Values sent between devices are 32-bit elements; how exact they have to be, the bound alone decides.
No kernel may reach another device: no remote copies, remote signals or barrier semaphores. Data moves between devices by JAX's collectives and lax.ppermute only.
A program may use at most 64 MiB of HBM per device.

```python
import math
import jax
import jax.numpy as jnp
import numpy as np
from jax import lax

NX = 240
NY = 240
NZ = 224
NH = 18
PAIRS = 171
SPECIES = 4
ATOMS = 256
BANDS = 512
GW = 32768
STK = 8
STICKS = 4096
BLOCK_STICKS = 256
NXB = 15


def draw_stick_columns(key, part):
    groups = STICKS // BLOCK_STICKS
    devices = BLOCK_STICKS // STK
    group_keys = jax.random.split(jax.random.fold_in(key, 11), groups)

    def one_group(group_key):
        perm_key, count_key, full_key = jax.random.split(group_key, 3)
        chosen = jax.random.permutation(perm_key, NXB * NY)[:BLOCK_STICKS].astype(jnp.int32).reshape(devices, STK)
        live_count = jax.random.randint(count_key, (devices,), 1, STK // 2 + 1)
        fullest = jax.random.randint(full_key, (), 0, devices)
        live_count = jnp.where(jnp.arange(devices) == fullest, STK, live_count)
        slot_index = jnp.arange(STK)[None, :]
        return jnp.where(slot_index < live_count[:, None], chosen, -1).reshape(-1)
    return jax.vmap(one_group)(group_keys).reshape(-1).astype(jnp.int32)


def place_ends(values, own_key, least, high):
    longest = values.shape.index(max(values.shape))
    spots = []
    for shift in (0, 1):
        where = [jax.random.randint(jax.random.fold_in(own_key, axis), (), 0, length) for axis, length in enumerate(values.shape)]
        where[longest] = (where[longest] + shift) % values.shape[longest]
        spots.append(tuple(where))
    return values.at[spots[0]].set(least).at[spots[1]].set(high)


def levels(stream_key, extent, shards, low, top_value):
    level = 1.0
    for position, parts in shards:
        heights = jax.random.uniform(jax.random.fold_in(jax.random.fold_in(stream_key, 6), position), (parts,), jnp.float32, low / len(shards), top_value / len(shards))
        level = level * jnp.repeat(jnp.exp(heights), extent[position] // parts).reshape((-1,) + (1,) * (len(extent) - 1 - position))
    return level


def centred(key, extent, spread, limit, cuts=(), held_as=jnp.bfloat16):
    values = jax.random.normal(key, extent, jnp.float32) * spread
    if len(cuts) > 0:
        values = levels(key, extent, cuts, -0.22, 0.18) * values
    return jnp.clip(values, min=-limit, max=limit).astype(held_as)


def setup_inputs(seed: int = 0) -> dict:
    key_of = jax.random.split(jax.random.key(seed), 9)
    return {
        "waves": centred(key_of[0], (2, BANDS, GW), 1.0, 6.0, ((1, 16), (2, 32))),
        "occupations": jnp.clip(jnp.exp(math.log(0.0078125) - 2.9957323 * jax.random.uniform(key_of[1], (BANDS,), jnp.float32) ** levels(key_of[1], (BANDS,), ((0, 16),), -0.2, 0.2)), 0.000390625, 0.0078125),
        "beta_table": centred(key_of[2], (SPECIES * NH, GW), (2 * GW) ** -0.5, 0.0234375, ((1, 32),), jnp.float32),
        "wave_miller": place_ends(jax.random.randint(key_of[3], (3, GW), 0, min(NX, min(NY, NZ))), jax.random.fold_in(key_of[3], 1), 0, (min(NX, min(NY, NZ))) - 1).astype(jnp.int32),
        "atom_kinds": place_ends(jax.random.randint(key_of[4], (ATOMS,), 0, SPECIES), jax.random.fold_in(key_of[4], 1), 0, SPECIES - 1).astype(jnp.int32),
        "atom_sites": place_ends(jax.random.randint(key_of[5], (3, ATOMS), 0, min(NX, min(NY, NZ))), jax.random.fold_in(key_of[5], 1), 0, (min(NX, min(NY, NZ))) - 1).astype(jnp.int32),
        "aug_table": centred(key_of[6], (SPECIES * PAIRS, STICKS * NZ), ((40.0 * ATOMS * STICKS * NZ) ** -0.5), 0.00015258789, ((1, 512),)),
        "stick_columns": draw_stick_columns(jax.random.fold_in(key_of[8], 71), 0),
    }


highest = lax.Precision.HIGHEST


def pair_tables(proj_count):
    ell_values = np.array([0, 0] + [1] * 6 + [2] * 10)
    pair_first, pair_second = np.triu_indices(proj_count)
    factors = np.where(pair_first == pair_second, 1.0, 2.0).astype(np.float32)
    parity = ((ell_values[pair_first] + ell_values[pair_second]) % 2).astype(np.float32)
    return pair_first * proj_count + pair_second, factors, parity


def phase_coefficients():
    ell_values = np.array([0, 0] + [1] * 6 + [2] * 10)
    coef_real = np.array([1.0, 0.0, -1.0])[ell_values]
    coef_imag = np.array([0.0, -1.0, 0.0])[ell_values]
    return jnp.asarray(coef_real, jnp.float32), jnp.asarray(coef_imag, jnp.float32)


def phase_angle(site_block, first, second, third):
    turn_count = ((site_block[0][:, None] * first[None, :]) % NX) * (NY * NZ)
    turn_count = turn_count + ((site_block[1][:, None] * second[None, :]) % NY) * (NX * NZ)
    turn_count = turn_count + ((site_block[2][:, None] * third[None, :]) % NZ) * (NX * NY)
    turn_count = (turn_count % (NX * NY * NZ)).astype(jnp.int32)
    angle_value = turn_count.astype(jnp.float32) * (2.0 * np.pi / (NX * NY * NZ))
    return jnp.cos(angle_value), -jnp.sin(angle_value)


def structure_factor(site_block, miller):
    return phase_angle(site_block, miller[0], miller[1], miller[2])


def projector_rows(site_block, kinds_block, beta_table, wave_miller):
    struct_re, struct_im = structure_factor(site_block, wave_miller)
    kind_onehot = (kinds_block[:, None] == jnp.arange(SPECIES, dtype=jnp.int32)[None, :]).astype(jnp.float32)
    table_three = beta_table.reshape(SPECIES, NH, -1)
    radial = jnp.einsum("as,sig->aig", kind_onehot, table_three, precision=highest)
    coef_real, coef_imag = phase_coefficients()
    part_re = radial * struct_re[:, None, :]
    part_im = radial * struct_im[:, None, :]
    vkb_re = coef_real[None, :, None] * part_re - coef_imag[None, :, None] * part_im
    vkb_im = coef_real[None, :, None] * part_im + coef_imag[None, :, None] * part_re
    return vkb_re.astype(jnp.bfloat16), vkb_im.astype(jnp.bfloat16)


def augment_weights(becsum, atom_kinds):
    pair_index, factors, parity = pair_tables(NH)
    kind_onehot = (atom_kinds[None, :] == jnp.arange(SPECIES, dtype=jnp.int32)[:, None]).astype(jnp.float32)
    parity_col = jnp.asarray(parity, jnp.float32)[:, None]
    even_rows = becsum.T * (1.0 - parity_col)
    odd_rows = -(becsum.T * parity_col)
    real_part = kind_onehot[:, None, :] * even_rows[None, :, :]
    imag_part = kind_onehot[:, None, :] * odd_rows[None, :, :]
    stacked = jnp.concatenate([real_part, imag_part], axis=2)
    return stacked.reshape(-1, stacked.shape[2]).astype(jnp.bfloat16)


def dense_augmentation(coefficients, atom_sites, column_x, column_y):
    slot_total = column_x.shape[0]
    zeros_z = jnp.zeros((1, NZ), jnp.int32)
    flat_x = (column_x[:, None] + zeros_z).reshape(-1).astype(jnp.int32)
    flat_y = (column_y[:, None] + zeros_z).reshape(-1).astype(jnp.int32)
    flat_z = (jnp.zeros((slot_total, 1), jnp.int32) + jnp.arange(NZ, dtype=jnp.int32)[None, :]).reshape(-1)
    struct_re, struct_im = phase_angle(atom_sites, flat_x, flat_y, flat_z)
    atom_total = coefficients.shape[0] // 2
    amp_re = coefficients[:atom_total]
    amp_im = coefficients[atom_total:]
    aug_re = jnp.sum(amp_re * struct_re - amp_im * struct_im, axis=0)
    aug_im = jnp.sum(amp_re * struct_im + amp_im * struct_re, axis=0)
    return aug_re.reshape(slot_total, NZ), aug_im.reshape(slot_total, NZ)


def reference(waves, occupations, beta_table, wave_miller, atom_kinds, atom_sites, aug_table, stick_columns):
    block_atoms = math.gcd(ATOMS, 8)
    wave_re = waves[0].astype(jnp.float32).T
    wave_im = waves[1].astype(jnp.float32).T

    def project_block(block_index):
        first_atom = block_index * block_atoms
        site_block = lax.dynamic_slice_in_dim(atom_sites, first_atom, block_atoms, 1)
        kinds_block = lax.dynamic_slice_in_dim(atom_kinds, first_atom, block_atoms, 0)
        vkb_re, vkb_im = projector_rows(site_block, kinds_block, beta_table, wave_miller)
        vkb_re = vkb_re.reshape(block_atoms * NH, -1).astype(jnp.float32)
        vkb_im = vkb_im.reshape(block_atoms * NH, -1).astype(jnp.float32)
        proj_re = jnp.dot(vkb_re, wave_re, precision=highest, preferred_element_type=jnp.float32) + jnp.dot(vkb_im, wave_im, precision=highest, preferred_element_type=jnp.float32)
        proj_im = jnp.dot(vkb_re, wave_im, precision=highest, preferred_element_type=jnp.float32) - jnp.dot(vkb_im, wave_re, precision=highest, preferred_element_type=jnp.float32)
        return proj_re.reshape(block_atoms, NH, -1), proj_im.reshape(block_atoms, NH, -1)

    becp_re, becp_im = lax.map(project_block, jnp.arange(ATOMS // block_atoms, dtype=jnp.int32))
    becp_re = becp_re.reshape(ATOMS, NH, -1)
    becp_im = becp_im.reshape(ATOMS, NH, -1)
    full_square = jnp.einsum("aic,ajc->aij", becp_re * occupations[None, None, :], becp_re, precision=highest)
    full_square = full_square + jnp.einsum("aic,ajc->aij", becp_im * occupations[None, None, :], becp_im, precision=highest)
    pair_index, factors, parity = pair_tables(NH)
    becsum = full_square.reshape(ATOMS, NH * NH)[:, pair_index] * factors[None, :]

    aug_weights = augment_weights(becsum, atom_kinds).astype(jnp.float32)
    stick_block = math.gcd(STICKS, 16)

    def dense_block(block_index):
        first_stick = block_index * stick_block
        columns = lax.dynamic_slice_in_dim(stick_columns, first_stick, stick_block, 0)
        table_block = lax.dynamic_slice_in_dim(aug_table, first_stick * NZ, stick_block * NZ, 1).astype(jnp.float32)
        stick_ids = first_stick + jnp.arange(stick_block, dtype=jnp.int32)
        column_x = (stick_ids // BLOCK_STICKS) * NXB + columns // NY
        column_y = columns % NY
        coefficients = jnp.dot(aug_weights.T, table_block, precision=highest, preferred_element_type=jnp.float32)
        aug_re, aug_im = dense_augmentation(coefficients, atom_sites, column_x, column_y)
        flat_rows = jnp.where(columns < 0, NX * NY, column_x * NY + column_y).astype(jnp.int32)
        return aug_re, aug_im, flat_rows

    aug_re, aug_im, flat_rows = lax.map(dense_block, jnp.arange(STICKS // stick_block, dtype=jnp.int32))
    flat_rows = flat_rows.reshape(-1)
    grid_re = jnp.zeros((NX * NY, NZ), jnp.float32).at[flat_rows].add(aug_re.reshape(-1, NZ), mode="drop")
    grid_im = jnp.zeros((NX * NY, NZ), jnp.float32).at[flat_rows].add(aug_im.reshape(-1, NZ), mode="drop")
    grid_values = lax.complex(grid_re, grid_im).reshape(NX, NY, NZ)
    density_field = jnp.fft.ifftn(grid_values) * (NX * NY * NZ)
    density_field = jnp.transpose(density_field, (2, 1, 0))
    return jnp.stack([jnp.real(density_field), jnp.imag(density_field)]).astype(jnp.float32)
```

```python
import functools

import jax
import jax.numpy as jnp
import numpy as np
from jax import lax
from jax.experimental import pallas as pl
from jax.experimental.pallas import tpu as pltpu
from jax.sharding import PartitionSpec as P

NX = 240
NY = 240
NZ = 224
NH = 18
PAIRS = 171
SPECIES = 4
ATOMS = 256
HALF = NH // 2
F32 = jnp.float32
BF16 = jnp.bfloat16
VMEM = pltpu.VMEM
SMEM = pltpu.SMEM


def turn_polynomials():
    nodes = np.cos(np.pi * (np.arange(400) + 0.5) / 400)
    squares = 0.125 + 0.125 * nodes
    turns = np.sqrt(squares)
    sine = np.polynomial.chebyshev.Chebyshev.fit(
        squares, np.sin(2 * np.pi * turns) / turns, 6, domain=[0, 0.25]
    )
    cosine = np.polynomial.chebyshev.Chebyshev.fit(
        squares, np.cos(2 * np.pi * turns), 7, domain=[0, 0.25]
    )
    poly = np.polynomial.polynomial.Polynomial
    return (
        [float(v) for v in sine.convert(kind=poly).coef],
        [float(v) for v in cosine.convert(kind=poly).coef],
    )


SINE_TERMS, COSINE_TERMS = turn_polynomials()


def horner(terms, value):
    total = jnp.full_like(value, terms[-1])
    for term in terms[-2::-1]:
        total = total * value + term
    return total


def turn_waves(turns):
    square = turns * turns
    return horner(COSINE_TERMS, square), turns * horner(SINE_TERMS, square)


def turns_of(count, length):
    return (count - length * jnp.round(count * (1.0 / length))) * (1.0 / length)


def site_waves(site_cols, miller_rows):
    in_plane = site_cols[0] * miller_rows[0] + site_cols[1] * miller_rows[1]
    turns = turns_of(in_plane, NX) + turns_of(site_cols[2] * miller_rows[2], NZ)
    return turn_waves(turns - jnp.round(turns))


def iota(shape, dim):
    return lax.broadcasted_iota(jnp.int32, shape, dim)


def split_two(value):
    high = value.astype(BF16)
    return high, (value - high.astype(F32)).astype(BF16)


def mm(left, right):
    return jnp.dot(left, right, preferred_element_type=F32)


def mm_nt(left, right):
    return lax.dot_general(left, right, (((1,), (1,)), ((), ())), preferred_element_type=F32)


def mm_three(left, right_high, right_low):
    high, low = split_two(left)
    return mm(high, right_high) + (mm(high, right_low) + mm(low, right_high))


def as_columns(rows):
    eye = (iota((ATOMS, ATOMS), 0) == iota((ATOMS, ATOMS), 1)).astype(F32).astype(BF16)
    return mm_nt(eye, rows.astype(BF16))


def atom_columns(sites_ref, kinds_ref):
    rows = jnp.concatenate(
        [
            sites_ref[...].astype(F32),
            kinds_ref[...].astype(F32),
            jnp.zeros((4, ATOMS), F32),
        ],
        axis=0,
    )
    return as_columns(rows)


def project_kernel(waves, beta, miller, kinds, sites, out, cos_s, sin_s, radial_s, wave_s, kind_s):
    g_count = beta.shape[1]
    step = pl.program_id(0)

    @pl.when(step == 0)
    def _():
        columns = atom_columns(sites, kinds)
        kind_s[...] = jnp.broadcast_to(columns[:, 3:4], (ATOMS, 128))
        site_cols = [columns[:, d : d + 1] for d in range(3)]
        for start in range(0, g_count, 256):
            rows = [miller[d : d + 1, start : start + 256].astype(F32) for d in range(3)]
            cosine, sine = site_waves(site_cols, rows)
            cos_s[:, start : start + 256] = cosine
            sin_s[:, start : start + 256] = sine
        table = beta[...]
        first = table.astype(BF16)
        rest = table - first.astype(F32)
        second = rest.astype(BF16)
        third = (rest - second.astype(F32)).astype(BF16)
        radial_s[...] = jnp.zeros(radial_s.shape, BF16)
        radial_s[0:72] = first
        radial_s[80:152] = second
        radial_s[160:232] = third
        wave_re = waves[0].astype(F32)
        wave_im = waves[1].astype(F32)
        blank = jnp.zeros((64, g_count), F32)
        with_cos = jnp.concatenate([wave_re, wave_im], axis=0)
        with_sin = jnp.concatenate([-wave_im, wave_re], axis=0)
        wave_s[0] = jnp.concatenate([with_cos, blank], axis=0).T.astype(BF16)
        wave_s[1] = jnp.concatenate([with_sin, blank], axis=0).T.astype(BF16)
        wave_s[2] = jnp.concatenate([blank, with_cos], axis=0).T.astype(BF16)
        wave_s[3] = jnp.concatenate([blank, with_sin], axis=0).T.astype(BF16)

    lane = iota((ATOMS, 256), 1)
    table_row = jnp.where(lane >= 160, lane - 160, jnp.where(lane >= 80, lane - 80, lane))
    table_row = jnp.where(lane >= 240, -1, table_row).astype(F32)
    wanted = jnp.concatenate([kind_s[...], kind_s[...]], axis=1) * float(NH)
    total = None
    for which in range(2):
        pick = (table_row == wanted + (2 * step + which).astype(F32)).astype(F32).astype(BF16)
        for start in range(0, g_count, 256):
            span = slice(start, start + 256)
            radial = mm(pick, radial_s[:, span])
            part_cos = (radial * cos_s[:, span]).astype(BF16)
            part_sin = (radial * sin_s[:, span]).astype(BF16)
            part = mm(part_cos, wave_s[2 * which, span]) + mm(part_sin, wave_s[2 * which + 1, span])
            total = part if total is None else total + part
    out[...] = total.reshape(ATOMS // 8, 1, 8, 128)


def project(waves, beta, miller, kinds, sites):
    g_count = beta.shape[1]
    whole = lambda shape: pl.BlockSpec(shape, lambda i: (0,) * len(shape))
    return pl.pallas_call(
        project_kernel,
        grid=(HALF,),
        in_specs=[
            whole(waves.shape),
            whole(beta.shape),
            whole(miller.shape),
            whole((1, ATOMS)),
            whole(sites.shape),
        ],
        out_specs=pl.BlockSpec((ATOMS // 8, 1, 8, 128), lambda i: (0, i, 0, 0)),
        out_shape=jax.ShapeDtypeStruct((ATOMS // 8, HALF, 8, 128), F32),
        scratch_shapes=[
            VMEM((ATOMS, g_count), F32),
            VMEM((ATOMS, g_count), F32),
            VMEM((256, g_count), BF16),
            VMEM((4, g_count, 128), BF16),
            VMEM((ATOMS, 128), F32),
        ],
        name="project",
    )(waves, beta, miller, kinds.reshape(1, ATOMS), sites)


def pair_constants():
    ell = np.array([0, 0] + [1] * 6 + [2] * 10)
    first, second = np.triu_indices(NH)
    take = np.zeros((NH * 8, 256), np.float32)
    keep = np.zeros((NH, 256), np.float32)
    for p in range(PAIRS):
        take[second[p] * 8 : second[p] * 8 + 8, p] = 1.0
        keep[first[p], p] = 1.0 if first[p] == second[p] else 2.0
    lanes = np.zeros((8, 768), np.float32)
    lanes[:2] = -1.0
    for s in range(SPECIES):
        span = slice(s * PAIRS, (s + 1) * PAIRS)
        lanes[0, span] = np.arange(PAIRS)
        lanes[1, span] = s
        odd = (ell[first] + ell[second]) % 2
        lanes[2, span] = 1.0 - odd
        lanes[3, span] = -1.0 * odd
    return take, keep, lanes


def becsum_kernel(blocks, occ, take, keep, out):
    rows = []
    for pair in range(HALF):
        total = blocks[0, pair]
        for src in range(1, blocks.shape[0]):
            total = total + blocks[src, pair]
        if 1 <= pair <= 3:
            lane = iota((8, 128), 1)
            ahead = pltpu.roll(total, 96, 1)
            behind = pltpu.roll(total, 32, 1)
            total = jnp.where(lane % 64 < 32, -ahead, behind)
        elif pair >= 4:
            total = -total
        rows.append(total)
        rows.append(pltpu.roll(total, 64, 1))
    lane = iota((NH * 8, 128), 1)
    values = jnp.where(lane < 64, jnp.concatenate(rows, axis=0), 0.0)
    scaled = values * occ[...]
    square = lax.dot_general(
        scaled, values, (((1,), (1,)), ((), ())), precision=lax.Precision.HIGHEST,
        preferred_element_type=F32,
    )
    side = (NH * 8, NH * 8)
    square = jnp.where(iota(side, 0) % 8 == iota(side, 1) % 8, square, 0.0)
    high, low = split_two(square)
    lowest = (square - high.astype(F32) - low.astype(F32)).astype(BF16)
    chosen = mm(high, take[...]) + (mm(low, take[...]) + mm(lowest, take[...]))
    result = jnp.zeros((8, 256), F32)
    for i in range(NH):
        result = result + chosen[8 * i : 8 * i + 8] * keep[i : i + 1, :]
    for peer in range(out.shape[0]):
        out[peer] = result


def becsum_part(blocks, occupations, peers, take, keep):
    occ = jnp.tile(occupations, 4).reshape(1, 128)
    return pl.pallas_call(
        becsum_kernel,
        out_shape=jax.ShapeDtypeStruct((peers, 8, 256), F32),
        name="becsum",
    )(blocks, occ, jnp.asarray(take, BF16), jnp.asarray(keep))


def band_sum_kernel(parts, out):
    total = parts[0]
    for src in range(1, parts.shape[0]):
        total = total + parts[src]
    for peer in range(out.shape[0]):
        out[peer] = total


def band_sum(parts, peers):
    return pl.pallas_call(
        band_sum_kernel, out_shape=jax.ShapeDtypeStruct((peers, 8, 256), F32), name="band_sum"
    )(parts)


def augment_kernel(
    sticks, band, becsum, kinds, sites, lanes, cos_high, cos_low, sin_high, sin_low, table, out,
    weight_s, site_s, aug_s,
):
    step = pl.program_id(0)
    chunk = table.shape[1]

    @pl.when(step == 0)
    def _():
        columns = atom_columns(sites, kinds)
        for d in range(3):
            site_s[d] = jnp.broadcast_to(columns[:, d : d + 1], (ATOMS, 128))
        width = lanes.shape[1]
        spread = (iota((256, width), 0).astype(F32) == lanes[0:1, :]).astype(F32).astype(BF16)
        rounded = becsum[...].reshape(ATOMS, 256).astype(BF16)
        copies = mm(rounded, spread)
        mine = jnp.where(columns[:, 3:4] == lanes[1:2, :], copies, 0.0)
        weight_s[0:ATOMS] = (mine * lanes[2:3, :]).astype(BF16)
        weight_s[ATOMS:] = (mine * lanes[3:4, :]).astype(BF16)

    rows = table.shape[0]
    coeff = mm(weight_s[:, 0:rows], table[...])
    g_row = step * chunk + iota((1, chunk), 1)
    slot_row = jnp.zeros((1, chunk), jnp.int32)
    for slot in range(1, 8):
        slot_row = slot_row + (g_row >= slot * NZ).astype(jnp.int32)
    z_row = (g_row - slot_row * NZ).astype(F32)
    x_row = jnp.zeros((1, chunk), F32)
    y_row = jnp.zeros((1, chunk), F32)
    live_row = jnp.zeros((1, chunk), F32)
    for slot in range(8):
        column = sticks[slot]
        live = (column >= 0).astype(F32)
        column = jnp.maximum(column, 0)
        x_in_block = column // NY
        x_value = (band[0] * (NX // 16) + x_in_block).astype(F32)
        y_value = (column - x_in_block * NY).astype(F32)
        here = slot_row == slot
        x_row = jnp.where(here, x_value, x_row)
        y_row = jnp.where(here, y_value, y_row)
        live_row = jnp.where(here, live, live_row)
    reps = chunk // 128
    site_cols = [jnp.concatenate([site_s[d]] * reps, axis=1) for d in range(3)]
    cosine, sine = site_waves(site_cols, [x_row, y_row, z_row])
    amp_re = coeff[0:ATOMS]
    amp_im = coeff[ATOMS:]
    aug_re = jnp.sum(amp_re * cosine + amp_im * sine, axis=0, keepdims=True) * live_row
    aug_im = jnp.sum(amp_im * cosine - amp_re * sine, axis=0, keepdims=True) * live_row
    start = pl.multiple_of(step * chunk, chunk)
    aug_s[0:1, pl.ds(start, chunk)] = aug_re
    aug_s[1:2, pl.ds(start, chunk)] = aug_im

    @pl.when(step == pl.num_programs(0) - 1)
    def _():
        stick = [aug_s[0:1, s * NZ : (s + 1) * NZ] for s in range(8)]
        stick += [aug_s[1:2, s * NZ : (s + 1) * NZ] for s in range(8)]
        data = jnp.concatenate(stick, axis=0)
        by_cos = mm_three(data, cos_high[...], cos_low[...])
        by_sin = mm_three(data, sin_high[...], sin_low[...])
        out_re = by_cos[0:8] - by_sin[8:16]
        out_im = by_sin[0:8] + by_cos[8:16]
        sub = iota((8, 256), 0)
        x_info = jnp.zeros((8, 256), F32)
        y_info = jnp.zeros((8, 256), F32)
        for slot in range(8):
            column = jnp.maximum(sticks[slot], 0)
            x_in_block = column // NY
            x_info = jnp.where(sub == slot, x_in_block.astype(F32), x_info)
            y_info = jnp.where(sub == slot, (column - x_in_block * NY).astype(F32), y_info)
        lane = iota((8, 256), 1)
        out_re = jnp.where(lane < NZ, out_re, x_info)
        out_im = jnp.where(lane < NZ, out_im, y_info)
        turned = jnp.concatenate([out_re, out_im], axis=0).T
        out[...] = jnp.concatenate([turned[32 * j : 32 * j + 32] for j in range(8)], axis=1)


def z_tables():
    z = np.arange(NZ)
    plane = np.zeros(256, np.int64)
    plane[:NZ] = 7 * (np.arange(NZ) % 32) + np.arange(NZ) // 32
    angle = 2 * np.pi * ((z[:, None] * plane[None, :]) % NZ) / NZ
    live = (np.arange(256) < NZ)[None, :]
    return np.cos(angle) * live, np.sin(angle) * live


def halves(table):
    table = np.asarray(table, np.float32)
    high = table.astype(jnp.bfloat16)
    return jnp.asarray(high), jnp.asarray((table - high.astype(np.float32)).astype(jnp.bfloat16))


def augment(sticks, band, becsum, kinds, sites, lanes, table):
    rows, count = table.shape
    chunk = 256
    cosine, sine = z_tables()
    cos_high, cos_low = halves(cosine)
    sin_high, sin_low = halves(sine)
    whole = lambda shape: pl.BlockSpec(shape, lambda i: (0,) * len(shape))
    scalar = pl.BlockSpec(memory_space=SMEM)
    return pl.pallas_call(
        augment_kernel,
        grid=(count // chunk,),
        in_specs=[
            scalar,
            scalar,
            whole(becsum.shape),
            whole((1, ATOMS)),
            whole(sites.shape),
            whole(lanes.shape),
        ]
        + [whole((NZ, 256))] * 4
        + [pl.BlockSpec((rows, chunk), lambda i: (0, i))],
        out_specs=whole((32, 128)),
        out_shape=jax.ShapeDtypeStruct((32, 128), F32),
        scratch_shapes=[
            VMEM((2 * ATOMS, lanes.shape[1]), BF16),
            VMEM((3, ATOMS, 128), F32),
            VMEM((8, count), F32),
        ],
        name="augment",
    )(
        sticks, band, becsum, kinds.reshape(1, ATOMS), sites, jnp.asarray(lanes),
        cos_high, cos_low, sin_high, sin_low, table,
    )


def spread_constants():
    spread = np.zeros((8, 128, 256), np.float32)
    for slot in range(8):
        for j in range(8):
            for part in range(2):
                row = j * 16 + part * 8 + slot
                spread[slot, row, part * 128 + j * 16 : part * 128 + j * 16 + 16] = 1.0
    return spread


def y_kernel(values, spread, out):
    high, low = split_two(values[...].reshape(32, 128))
    parts = []
    for slot in range(8):
        parts.append(mm(high, spread[slot]) + mm(low, spread[slot]))
    wide = jnp.concatenate(parts, axis=0)
    y_col = wide[:, 240:241]
    source = jnp.where(iota((8, 256), 0) == 0, 112, 240)
    pick = (iota((8, 256), 1) == source).astype(F32).astype(BF16)
    info = mm_nt(pick, wide.astype(BF16))
    x_t = info[0:1, :]
    y_t = info[1:2, :]
    lane = iota((256, 128), 1)
    cosine, sine = turn_waves(turns_of(y_col * (lane % 16).astype(F32), NY))
    real = wide[:, 0:128]
    imag = wide[:, 128:256]
    keep = lane < 112
    new_re = jnp.where(keep, real * cosine - imag * sine, 0.0)
    new_im = jnp.where(keep, real * sine + imag * cosine, 0.0)
    right = jnp.concatenate(
        [
            jnp.concatenate([new_re, new_im], axis=1),
            jnp.concatenate([-new_im, new_re], axis=1),
        ],
        axis=0,
    )
    line = iota((256, 256), 0)
    here = (line % 16).astype(F32) == x_t
    far_cos, far_sin = turn_waves(turns_of(y_t * (line // 16).astype(F32), 16))
    left = jnp.concatenate([jnp.where(here, far_cos, 0.0), jnp.where(here, far_sin, 0.0)], axis=1)
    right_high, right_low = split_two(right)
    out[...] = mm_three(left, right_high, right_low).reshape(16, 16, 256)


def y_transform(values):
    spread = jnp.asarray(spread_constants(), BF16)
    return pl.pallas_call(
        y_kernel, out_shape=jax.ShapeDtypeStruct((16, 16, 256), F32), name="y_transform"
    )(values, spread)


def x_tables():
    row = np.arange(256)
    x_in = 15 * (row // 16) + row % 16
    x_out = np.arange(256)
    angle = 2 * np.pi * ((x_in[:, None] * x_out[None, :]) % NX) / NX
    live = (row % 16 < 15)[:, None] & (x_out < NX)[None, :]
    return np.cos(angle) * live, np.sin(angle) * live


def x_kernel(values, cos_high, cos_low, sin_high, sin_low, out):
    turned = values[...].reshape(256, 256).T
    by_cos = mm_three(turned, cos_high[...], cos_low[...])
    by_sin = mm_three(turned, sin_high[...], sin_low[...])
    real = by_cos[0:128] - by_sin[128:256]
    imag = by_sin[0:128] + by_cos[128:256]
    for j in range(7):
        out[0, j] = real[16 * j : 16 * j + 15, 0:NX]
        out[1, j] = imag[16 * j : 16 * j + 15, 0:NX]


def x_transform(values):
    cosine, sine = x_tables()
    return pl.pallas_call(
        x_kernel, out_shape=jax.ShapeDtypeStruct((2, 7, 15, NX), F32), name="x_transform"
    )(values, *halves(cosine), *halves(sine))


def exchange(value, axis):
    return lax.all_to_all(value, axis, 0, 0, tiled=True)


def on_device(
    waves, occupations, beta_table, wave_miller, atom_kinds, atom_sites, aug_table, stick_columns
):
    take, keep, lanes = pair_constants()
    bands = lax.axis_size("band")
    groups = lax.axis_size("ga")
    band = lax.axis_index("band").reshape(1)
    pieces = project(waves, beta_table, wave_miller, atom_kinds, atom_sites)
    pieces = exchange(pieces, "ga")
    part = becsum_part(pieces, occupations, bands, take, keep)
    summed = band_sum(exchange(part, "band"), groups)
    becsum = exchange(summed, "ga")
    columns = augment(stick_columns, band, becsum, atom_kinds, atom_sites, lanes, aug_table)
    planes = y_transform(exchange(columns.reshape(32, 1, 128), "ga"))
    return x_transform(exchange(planes, "band"))


def solution(mesh):
    in_specs = (
        P(None, "band", "ga"),
        P("band"),
        P(None, "ga"),
        P(None, "ga"),
        P(),
        P(),
        P(None, ("band", "ga")),
        P(("band", "ga")),
    )
    out_specs = P(None, "ga", "band", None)
    return jax.shard_map(
        on_device, mesh=mesh, in_specs=in_specs, out_specs=out_specs, check_vma=False
    )
```

```python
import functools

import jax
import jax.numpy as jnp
import numpy as np
from jax import lax
from jax.experimental import pallas as pl
from jax.experimental.pallas import tpu as pltpu
from jax.sharding import PartitionSpec as P

NX = 240
NY = 240
NZ = 224
NH = 18
PAIRS = 171
SPECIES = 4
ATOMS = 256
HALF = NH // 2
PAIRS_A_STEP = 3
F32 = jnp.float32
BF16 = jnp.bfloat16
VMEM = pltpu.VMEM
SMEM = pltpu.SMEM
MIB = 1 << 20


def turn_polynomials():
    nodes = np.cos(np.pi * (np.arange(400) + 0.5) / 400)
    squares = 0.125 + 0.125 * nodes
    turns = np.sqrt(squares)
    sine = np.polynomial.chebyshev.Chebyshev.fit(
        squares, np.sin(2 * np.pi * turns) / turns, 6, domain=[0, 0.25]
    )
    cosine = np.polynomial.chebyshev.Chebyshev.fit(
        squares, np.cos(2 * np.pi * turns), 7, domain=[0, 0.25]
    )
    poly = np.polynomial.polynomial.Polynomial
    return (
        [float(v) for v in sine.convert(kind=poly).coef],
        [float(v) for v in cosine.convert(kind=poly).coef],
    )


SINE_TERMS, COSINE_TERMS = turn_polynomials()


def horner(terms, value):
    total = jnp.full_like(value, terms[-1])
    for term in terms[-2::-1]:
        total = total * value + term
    return total


def turn_waves(turns):
    square = turns * turns
    return horner(COSINE_TERMS, square), turns * horner(SINE_TERMS, square)


def turns_of(count, length):
    return (count - length * jnp.round(count * (1.0 / length))) * (1.0 / length)


def site_waves(site_cols, miller_rows):
    in_plane = site_cols[0] * miller_rows[0] + site_cols[1] * miller_rows[1]
    turns = turns_of(in_plane, NX) + turns_of(site_cols[2] * miller_rows[2], NZ)
    return turn_waves(turns - jnp.round(turns))


def iota(shape, dim):
    return lax.broadcasted_iota(jnp.int32, shape, dim)


def split_two(value):
    high = value.astype(BF16)
    return high, (value - high.astype(F32)).astype(BF16)


def mm(left, right):
    return jnp.dot(left, right, preferred_element_type=F32)


def mm_nt(left, right):
    return lax.dot_general(left, right, (((1,), (1,)), ((), ())), preferred_element_type=F32)


def mm_three(left, right_high, right_low):
    high, low = split_two(left)
    return mm(high, right_high) + (mm(high, right_low) + mm(low, right_high))


def as_columns(rows):
    eye = (iota((ATOMS, ATOMS), 0) == iota((ATOMS, ATOMS), 1)).astype(F32).astype(BF16)
    return mm_nt(eye, rows.astype(BF16))


def atom_columns(sites_ref, kinds_ref):
    rows = jnp.concatenate(
        [
            sites_ref[...].astype(F32),
            kinds_ref[...].astype(F32),
            jnp.zeros((4, ATOMS), F32),
        ],
        axis=0,
    )
    return as_columns(rows)


def project_kernel(waves, beta, miller, kinds, sites, out, site_s, wave_s, phi_s):
    g_count = beta.shape[1]
    step = pl.program_id(0)

    @pl.when(step == 0)
    def _():
        site_rows = [sites[d : d + 1, :].astype(F32) for d in range(3)]
        for start in range(0, g_count, 256):
            rows = [miller[:, start : start + 256].astype(F32), jnp.zeros((5, 256), F32)]
            columns = as_columns(jnp.concatenate(rows, axis=0))
            cosine, sine = site_waves([columns[:, d : d + 1] for d in range(3)], site_rows)
            site_s[start : start + 256, 0:ATOMS] = cosine.astype(BF16)
            site_s[start : start + 256, ATOMS:] = sine.astype(BF16)
        wave_s[0:32] = waves[0].astype(F32)
        wave_s[32:64] = waves[1].astype(F32)

    kind = jnp.concatenate([kinds[...], kinds[...]], axis=1)

    def fill(slot, projector):
        for species in range(SPECIES):
            row = beta[pl.ds(species * NH + projector, 1), :]
            phi_s[slot, species * 64 : species * 64 + 64] = (row * wave_s[...]).astype(BF16)

    count = 2 * out.shape[1]
    first = count * step
    fill(0, first)
    both = []
    for index in range(count):
        if index + 1 < count:
            fill(index + 1, first + index + 1)
        every = mm(phi_s[index], site_s[...])
        mine = every[192:256]
        for species in range(3):
            mine = jnp.where(kind == species, every[species * 64 : species * 64 + 64], mine)
        both.append(mine[0:32, 0:ATOMS] - mine[32:64, ATOMS:])
        both.append(mine[32:64, 0:ATOMS] + mine[0:32, ATOMS:])
        if index % 2:
            turned = jnp.concatenate(both, axis=0).T
            out[:, index // 2] = turned.reshape(ATOMS // 8, 8, 128)
            both = []


def project(waves, beta, miller, kinds, sites):
    g_count = beta.shape[1]
    whole = lambda shape: pl.BlockSpec(shape, lambda i: (0,) * len(shape))
    return pl.pallas_call(
        project_kernel,
        grid=(HALF // PAIRS_A_STEP,),
        in_specs=[
            whole(waves.shape),
            whole(beta.shape),
            whole(miller.shape),
            whole((1, ATOMS)),
            whole(sites.shape),
        ],
        out_specs=pl.BlockSpec((ATOMS // 8, PAIRS_A_STEP, 8, 128), lambda i: (0, i, 0, 0)),
        out_shape=jax.ShapeDtypeStruct((ATOMS // 8, HALF, 8, 128), F32),
        scratch_shapes=[
            VMEM((g_count, 2 * ATOMS), BF16),
            VMEM((64, g_count), F32),
            VMEM((2 * PAIRS_A_STEP, 256, g_count), BF16),
        ],
        name="project",
    )(waves, beta, miller, kinds.reshape(1, ATOMS), sites)


def pair_constants():
    ell = np.array([0, 0] + [1] * 6 + [2] * 10)
    first, second = np.triu_indices(NH)
    take = np.zeros((NH * 8, 256), np.float32)
    keep = np.zeros((NH, 256), np.float32)
    for p in range(PAIRS):
        take[second[p] * 8 : second[p] * 8 + 8, p] = 1.0
        keep[first[p], p] = 1.0 if first[p] == second[p] else 2.0
    lanes = np.zeros((8, 768), np.float32)
    lanes[:2] = -1.0
    for s in range(SPECIES):
        span = slice(s * PAIRS, (s + 1) * PAIRS)
        lanes[0, span] = np.arange(PAIRS)
        lanes[1, span] = s
        odd = (ell[first] + ell[second]) % 2
        lanes[2, span] = 1.0 - odd
        lanes[3, span] = -1.0 * odd
    return take, keep, lanes


def becsum_kernel(blocks, occ, take, keep, out):
    rows = []
    for pair in range(HALF):
        total = blocks[0, pair]
        for src in range(1, blocks.shape[0]):
            total = total + blocks[src, pair]
        if 1 <= pair <= 3:
            lane = iota((8, 128), 1)
            ahead = pltpu.roll(total, 96, 1)
            behind = pltpu.roll(total, 32, 1)
            total = jnp.where(lane % 64 < 32, -ahead, behind)
        elif pair >= 4:
            total = -total
        rows.append(total)
        rows.append(pltpu.roll(total, 64, 1))
    lane = iota((NH * 8, 128), 1)
    values = jnp.where(lane < 64, jnp.concatenate(rows, axis=0), 0.0)
    scaled = values * occ[...]
    square = lax.dot_general(
        scaled, values, (((1,), (1,)), ((), ())), precision=lax.Precision.HIGHEST,
        preferred_element_type=F32,
    )
    side = (NH * 8, NH * 8)
    square = jnp.where(iota(side, 0) % 8 == iota(side, 1) % 8, square, 0.0)
    high, low = split_two(square)
    lowest = (square - high.astype(F32) - low.astype(F32)).astype(BF16)
    chosen = mm(high, take[...]) + (mm(low, take[...]) + mm(lowest, take[...]))
    result = jnp.zeros((8, 256), F32)
    for i in range(NH):
        result = result + chosen[8 * i : 8 * i + 8] * keep[i : i + 1, :]
    tails = result[0:4, 128:256] + pltpu.roll(result[4:8, 128:256], 64, 1)
    packed = jnp.concatenate([result[0:4, 0:128], tails, result[4:8, 0:128]], axis=1)
    for peer in range(out.shape[0]):
        out[peer] = packed


def becsum_part(blocks, occupations, peers, take, keep):
    occ = jnp.tile(occupations, 4).reshape(1, 128)
    return pl.pallas_call(
        becsum_kernel,
        in_specs=resident(4),
        out_shape=jax.ShapeDtypeStruct((peers, 4, 384), F32),
        name="becsum",
        compiler_params=pltpu.CompilerParams(vmem_limit_bytes=12 * MIB),
    )(on_chip(blocks), on_chip(occ), on_chip(jnp.asarray(take, BF16)), on_chip(jnp.asarray(keep)))


def band_sum_kernel(parts, out):
    total = parts[0]
    for src in range(1, parts.shape[0]):
        total = total + parts[src]
    for peer in range(out.shape[0]):
        out[peer] = total


def band_sum(parts, peers):
    return pl.pallas_call(
        band_sum_kernel,
        in_specs=resident(1),
        out_shape=jax.ShapeDtypeStruct((peers, 4, 384), F32),
        name="band_sum",
        compiler_params=pltpu.CompilerParams(vmem_limit_bytes=8 * MIB),
    )(on_chip(parts))


def slot_column(sticks, slot):
    column = jnp.maximum(sticks[slot], 0)
    x_in_block = column // NY
    return x_in_block, column - x_in_block * NY


def structure_kernel(sticks, band, kinds, sites, out, kind_out, site_s):
    step = pl.program_id(0)
    chunk = out.shape[2]

    @pl.when(step == 0)
    def _():
        line = iota((ATOMS, ATOMS), 0)
        atom = line % 128 // 4 * 8 + line // 128 * 4 + line % 4
        order = (iota((ATOMS, ATOMS), 1) == atom).astype(F32).astype(BF16)
        rows = [sites[...].astype(F32), kinds[...].astype(F32), jnp.zeros((4, ATOMS), F32)]
        columns = mm_nt(order, jnp.concatenate(rows, axis=0).astype(BF16))
        for d in range(3):
            site_s[d] = jnp.broadcast_to(columns[:, d : d + 1], (ATOMS, 128))
        kind_out[...] = jnp.broadcast_to(columns[:, 3:4], (ATOMS, 128))

    g_row = step * chunk + iota((1, chunk), 1)
    slot_row = jnp.zeros((1, chunk), jnp.int32)
    for slot in range(1, 8):
        slot_row = slot_row + (g_row >= slot * NZ).astype(jnp.int32)
    z_row = (g_row - slot_row * NZ).astype(F32)
    x_row = jnp.zeros((1, chunk), F32)
    y_row = jnp.zeros((1, chunk), F32)
    live_row = jnp.zeros((1, chunk), F32)
    for slot in range(8):
        x_in_block, y_value = slot_column(sticks, slot)
        x_value = band[0] * (NX // 16) + x_in_block
        here = slot_row == slot
        x_row = jnp.where(here, x_value.astype(F32), x_row)
        y_row = jnp.where(here, y_value.astype(F32), y_row)
        live_row = jnp.where(here, (sticks[slot] >= 0).astype(F32), live_row)
    reps = chunk // 128
    site_cols = [jnp.concatenate([site_s[d]] * reps, axis=1) for d in range(3)]
    cosine, sine = site_waves(site_cols, [x_row, y_row, z_row])
    out[0] = cosine * live_row
    out[1] = sine * live_row


def structure(sticks, band, kinds, sites, count):
    chunk = 256
    whole = lambda shape: pl.BlockSpec(shape, lambda i: (0,) * len(shape))
    scalar = pl.BlockSpec(memory_space=SMEM)
    return pl.pallas_call(
        structure_kernel,
        grid=(count // chunk,),
        in_specs=[scalar, scalar, whole((1, ATOMS)), whole(sites.shape)],
        out_specs=[pl.BlockSpec((2, ATOMS, chunk), lambda i: (0, 0, i)), whole((ATOMS, 128))],
        out_shape=[
            jax.ShapeDtypeStruct((2, ATOMS, count), F32),
            jax.ShapeDtypeStruct((ATOMS, 128), F32),
        ],
        scratch_shapes=[VMEM((3, ATOMS, 128), F32)],
        cost_estimate=pl.CostEstimate(flops=60 * ATOMS * count, transcendentals=0, bytes_accessed=8 * ATOMS * count),
        name="structure",
    )(sticks, band, kinds.reshape(1, ATOMS), sites)


def augment_kernel(
    sticks, becsum, kinds, lanes, cos_high, cos_low, sin_high, sin_low, phases_far, table_far, out,
    aug_s, phases, table, sems,
):
    copies = []
    for index in range(table.shape[1] // 256):
        span = pl.ds(index * 256, 256)
        pair = [
            pltpu.make_async_copy(table_far.at[:, span], table.at[:, span], sems.at[0, index]),
            pltpu.make_async_copy(
                phases_far.at[:, :, span], phases.at[:, :, span], sems.at[1, index]
            ),
        ]
        for copy in pair:
            copy.start()
        copies.append(pair)
    width = lanes.shape[1]
    spread = (iota((256, width), 0).astype(F32) == lanes[0:1, :]).astype(F32).astype(BF16)
    packed = becsum[...].reshape(128, 384)
    tail = packed[:, 128:256]
    rounded = jnp.concatenate(
        [
            jnp.concatenate([packed[:, 0:128], tail], axis=1),
            jnp.concatenate([packed[:, 256:384], pltpu.roll(tail, 64, 1)], axis=1),
        ],
        axis=0,
    ).astype(BF16)
    mine = jnp.where(kinds[:, 0:1] == lanes[1:2, :], mm(rounded, spread), 0.0)
    rows = table.shape[0]
    even = (mine * lanes[2:3, :]).astype(BF16)[:, 0:rows]
    odd = (mine * lanes[3:4, :]).astype(BF16)[:, 0:rows]
    for start in range(0, table.shape[1], 256):
        span = slice(start, start + 256)
        for copy in copies[start // 256]:
            copy.wait()
        amp_re = mm(even, table[:, span])
        amp_im = mm(odd, table[:, span])
        cosine = phases[0, :, span]
        sine = phases[1, :, span]
        aug_s[0:1, span] = jnp.sum(amp_re * cosine + amp_im * sine, axis=0, keepdims=True)
        aug_s[1:2, span] = jnp.sum(amp_im * cosine - amp_re * sine, axis=0, keepdims=True)
    stick = [aug_s[0:1, s * NZ : (s + 1) * NZ] for s in range(8)]
    stick += [aug_s[1:2, s * NZ : (s + 1) * NZ] for s in range(8)]
    data = jnp.concatenate(stick, axis=0)
    by_cos = mm_three(data, cos_high[...], cos_low[...])
    by_sin = mm_three(data, sin_high[...], sin_low[...])
    out_re = by_cos[0:8] - by_sin[8:16]
    out_im = by_sin[0:8] + by_cos[8:16]
    sub = iota((8, 256), 0)
    x_info = jnp.zeros((8, 256), F32)
    y_info = jnp.zeros((8, 256), F32)
    for slot in range(8):
        x_in_block, y_value = slot_column(sticks, slot)
        x_info = jnp.where(sub == slot, x_in_block.astype(F32), x_info)
        y_info = jnp.where(sub == slot, y_value.astype(F32), y_info)
    lane = iota((8, 256), 1)
    out_re = jnp.where(lane < NZ, out_re, x_info)
    out_im = jnp.where(lane < NZ, out_im, y_info)
    turned = jnp.concatenate([out_re, out_im], axis=0).T
    out[...] = jnp.concatenate([turned[32 * j : 32 * j + 32] for j in range(8)], axis=1)


def z_tables():
    z = np.arange(NZ)
    plane = np.zeros(256, np.int64)
    plane[:NZ] = 7 * (np.arange(NZ) % 32) + np.arange(NZ) // 32
    angle = 2 * np.pi * ((z[:, None] * plane[None, :]) % NZ) / NZ
    live = (np.arange(256) < NZ)[None, :]
    return np.cos(angle) * live, np.sin(angle) * live


def halves(table):
    table = np.asarray(table, np.float32)
    high = table.astype(jnp.bfloat16)
    return jnp.asarray(high), jnp.asarray((table - high.astype(np.float32)).astype(jnp.bfloat16))


def augment(sticks, becsum, kinds, phases, lanes, table):
    cosine, sine = z_tables()
    constants = [on_chip(c) for c in (*halves(cosine), *halves(sine))]
    return pl.pallas_call(
        augment_kernel,
        in_specs=[pl.BlockSpec(memory_space=SMEM)]
        + resident(7)
        + [pl.BlockSpec(memory_space=pltpu.HBM)] * 2,
        out_shape=jax.ShapeDtypeStruct((32, 128), F32),
        scratch_shapes=[
            VMEM((8, table.shape[1]), F32),
            VMEM(phases.shape, F32),
            VMEM(table.shape, BF16),
            pltpu.SemaphoreType.DMA((2, table.shape[1] // 256)),
        ],
        name="augment",
    )(
        sticks, on_chip(becsum), on_chip(kinds), on_chip(jnp.asarray(lanes)), *constants, phases,
        table,
    )


def spread_constants():
    spread = np.zeros((8, 128, 256), np.float32)
    for slot in range(8):
        for j in range(8):
            for part in range(2):
                row = j * 16 + part * 8 + slot
                spread[slot, row, part * 128 + j * 16 : part * 128 + j * 16 + 16] = 1.0
    return spread


def y_kernel(values, spread, out):
    high, low = split_two(values[...].reshape(32, 128))
    parts = []
    for slot in range(8):
        parts.append(mm(high, spread[slot]) + mm(low, spread[slot]))
    wide = jnp.concatenate(parts, axis=0)
    y_col = wide[:, 240:241]
    source = jnp.where(iota((8, 256), 0) == 0, 112, 240)
    pick = (iota((8, 256), 1) == source).astype(F32).astype(BF16)
    info = mm_nt(pick, wide.astype(BF16))
    x_t = info[0:1, :]
    y_t = info[1:2, :]
    lane = iota((256, 128), 1)
    cosine, sine = turn_waves(turns_of(y_col * (lane % 16).astype(F32), NY))
    real = wide[:, 0:128]
    imag = wide[:, 128:256]
    keep = lane < 112
    new_re = jnp.where(keep, real * cosine - imag * sine, 0.0)
    new_im = jnp.where(keep, real * sine + imag * cosine, 0.0)
    right = jnp.concatenate(
        [
            jnp.concatenate([new_re, new_im], axis=1),
            jnp.concatenate([-new_im, new_re], axis=1),
        ],
        axis=0,
    )
    line = iota((256, 256), 0)
    here = (line % 16).astype(F32) == x_t
    far_cos, far_sin = turn_waves(turns_of(y_t * (line // 16).astype(F32), 16))
    left = jnp.concatenate([jnp.where(here, far_cos, 0.0), jnp.where(here, far_sin, 0.0)], axis=1)
    right_high, right_low = split_two(right)
    out[...] = mm_three(left, right_high, right_low).reshape(16, 16, 256)


def y_transform(values):
    spread = jnp.asarray(spread_constants(), BF16)
    return pl.pallas_call(
        y_kernel,
        in_specs=resident(2),
        out_shape=jax.ShapeDtypeStruct((16, 16, 256), F32),
        name="y_transform",
        compiler_params=pltpu.CompilerParams(vmem_limit_bytes=12 * MIB),
    )(on_chip(values), on_chip(spread))


def x_tables():
    row = np.arange(256)
    x_in = 15 * (row // 16) + row % 16
    x_out = np.arange(256)
    angle = 2 * np.pi * ((x_in[:, None] * x_out[None, :]) % NX) / NX
    live = (row % 16 < 15)[:, None] & (x_out < NX)[None, :]
    return np.cos(angle) * live, np.sin(angle) * live


def x_kernel(values, cos_high, cos_low, sin_high, sin_low, out):
    turned = values[...].reshape(256, 256).T
    by_cos = mm_three(turned, cos_high[...], cos_low[...])
    by_sin = mm_three(turned, sin_high[...], sin_low[...])
    real = by_cos[0:128] - by_sin[128:256]
    imag = by_sin[0:128] + by_cos[128:256]
    for j in range(7):
        out[j, :, 0, :] = real[16 * j : 16 * j + 15, 0:NX]
        out[j, :, 1, :] = imag[16 * j : 16 * j + 15, 0:NX]


def x_transform(values):
    cosine, sine = x_tables()
    constants = [on_chip(c) for c in (*halves(cosine), *halves(sine))]
    result = pl.pallas_call(
        x_kernel,
        in_specs=resident(5),
        out_shape=jax.ShapeDtypeStruct((7, 15, 2, NX), F32),
        name="x_transform",
        compiler_params=pltpu.CompilerParams(vmem_limit_bytes=12 * MIB),
    )(on_chip(values), *constants)
    return jnp.transpose(result, (2, 0, 1, 3))


def on_chip(value):
    return pltpu.with_memory_space_constraint(value, VMEM)


def resident(count):
    return [pl.BlockSpec(memory_space=VMEM)] * count


def exchange(value, axis):
    return lax.all_to_all(value, axis, 0, 0, tiled=True)


def on_device(
    waves, occupations, beta_table, wave_miller, atom_kinds, atom_sites, aug_table, stick_columns
):
    take, keep, lanes = pair_constants()
    bands = lax.axis_size("band")
    groups = lax.axis_size("ga")
    band = lax.axis_index("band").reshape(1)
    pieces = project(waves, beta_table, wave_miller, atom_kinds, atom_sites)
    phases, kind_columns = structure(
        stick_columns, band, atom_kinds, atom_sites, aug_table.shape[1]
    )
    pieces = exchange(pieces, "ga")
    part = becsum_part(pieces, occupations, bands, take, keep)
    summed = band_sum(exchange(part, "band"), groups)
    becsum = exchange(summed, "ga")
    columns = augment(stick_columns, becsum, kind_columns, phases, lanes, aug_table)
    planes = y_transform(exchange(columns.reshape(32, 1, 128), "ga"))
    return x_transform(exchange(planes, "band"))


def solution(mesh):
    in_specs = (
        P(None, "band", "ga"),
        P("band"),
        P(None, "ga"),
        P(None, "ga"),
        P(),
        P(),
        P(None, ("band", "ga")),
        P(("band", "ga")),
    )
    out_specs = P(None, "ga", "band", None)
    return jax.shard_map(
        on_device, mesh=mesh, in_specs=in_specs, out_specs=out_specs, check_vma=False
    )
```

```python
import math

import jax
import jax.numpy as jnp
import numpy as np
from jax import lax
from jax.experimental import pallas as pl
from jax.experimental.pallas import tpu as pltpu
from jax.sharding import PartitionSpec as P

NX = 240
NY = 240
NZ = 224
NH = 18
PAIRS = 171
SPECIES = 4
ATOMS = 256
HALF = NH // 2
PAIRS_A_STEP = 3
F32 = jnp.float32
BF16 = jnp.bfloat16
VMEM = pltpu.VMEM
SMEM = pltpu.SMEM
MIB = 1 << 20
AHEAD = 7


def turn_polynomials():
    nodes = np.cos(np.pi * (np.arange(400) + 0.5) / 400)
    squares = 0.125 + 0.125 * nodes
    turns = np.sqrt(squares)
    sine = np.polynomial.chebyshev.Chebyshev.fit(
        squares, np.sin(2 * np.pi * turns) / turns, 6, domain=[0, 0.25]
    )
    cosine = np.polynomial.chebyshev.Chebyshev.fit(
        squares, np.cos(2 * np.pi * turns), 6, domain=[0, 0.25]
    )
    poly = np.polynomial.polynomial.Polynomial
    return (
        [float(v) for v in sine.convert(kind=poly).coef],
        [float(v) for v in cosine.convert(kind=poly).coef],
    )


SINE_TERMS, COSINE_TERMS = turn_polynomials()


def horner(terms, value):
    total = jnp.full_like(value, terms[-1])
    for term in terms[-2::-1]:
        total = total * value + term
    return total


def turn_waves(turns):
    square = turns * turns
    return horner(COSINE_TERMS, square), turns * horner(SINE_TERMS, square)


def turns_of(count, length):
    return (count - length * jnp.round(count * (1.0 / length))) * (1.0 / length)


def site_waves(site_cols, miller_rows):
    parts = math.lcm(NX, NY, NZ)
    rows = [row * (parts // length) for row, length in zip(miller_rows, (NX, NY, NZ))]
    count = site_cols[0] * rows[0] + site_cols[1] * rows[1] + site_cols[2] * rows[2]
    return turn_waves(turns_of(count, parts))


def iota(shape, dim):
    return lax.broadcasted_iota(jnp.int32, shape, dim)


def split_two(value):
    high = value.astype(BF16)
    return high, (value - high.astype(F32)).astype(BF16)


def mm(left, right):
    return jnp.dot(left, right, preferred_element_type=F32)


def mm_nt(left, right):
    return lax.dot_general(left, right, (((1,), (1,)), ((), ())), preferred_element_type=F32)


def mm_three(left, right_high, right_low):
    high, low = split_two(left)
    return mm(high, right_high) + (mm(high, right_low) + mm(low, right_high))


def as_columns(rows):
    eye = (iota((ATOMS, ATOMS), 0) == iota((ATOMS, ATOMS), 1)).astype(F32).astype(BF16)
    return mm_nt(eye, rows.astype(BF16))


def species_order(sites, kinds, places):
    kind_row = kinds[...].astype(F32)
    every = [sites[...].astype(F32), kind_row, jnp.zeros((4, ATOMS), F32)]
    every = jnp.concatenate(every, axis=0).astype(BF16)
    eye = (iota((ATOMS, ATOMS), 0) == iota((ATOMS, ATOMS), 1)).astype(F32).astype(BF16)
    kind_col = mm_nt(eye, every)[:, 3:4]
    earlier = iota((ATOMS, ATOMS), 0) < iota((ATOMS, ATOMS), 1)
    ahead = (kind_col < kind_row) | ((kind_col == kind_row) & earlier)
    rank = jnp.sum(ahead.astype(F32), axis=0, keepdims=True)
    return every, (places.astype(F32) == rank).astype(F32).astype(BF16)


def project_kernel(
    waves, beta, miller, kinds, sites, out, kind_s, site_s, wave_s, phi_s, sum_s, entry_s
):
    g_count = beta.shape[1]
    half = ATOMS // 2
    step = pl.program_id(0)

    @pl.when(step == 0)
    def _():
        below = jnp.int32(0)
        last = jnp.int32(0)
        for species in range(SPECIES - 1):
            below = below + jnp.sum((kinds[...] == species).astype(jnp.int32))
            last = last + (below < half).astype(jnp.int32)
        for entry in range(SPECIES + 1):
            later = (entry > last).astype(jnp.int32)
            entry_s[0, entry] = entry - later
            entry_s[1, entry] = later
        every, order = species_order(sites, kinds, iota((ATOMS, ATOMS), 0))
        mine = mm_nt(every, order)
        for part in range(2):
            span = slice(part * half, part * half + half)
            kind_s[part, 0:1, 0:half] = mine[3:4, span]
            kind_s[part, 0:1, half:] = mine[3:4, span]
        site_rows = [mine[d : d + 1] for d in range(3)]
        for start in range(0, g_count, 256):
            rows = [miller[:, start : start + 256].astype(F32), jnp.zeros((5, 256), F32)]
            columns = as_columns(jnp.concatenate(rows, axis=0))
            cosine, sine = site_waves([columns[:, d : d + 1] for d in range(3)], site_rows)
            for part in range(2):
                span = slice(part * half, part * half + half)
                site_s[part, start : start + 256, 0:half] = cosine[:, span].astype(BF16)
                site_s[part, start : start + 256, half:] = sine[:, span].astype(BF16)
        wave_s[0:32] = waves[0].astype(F32)
        wave_s[32:64] = waves[1].astype(F32)

    count = 2 * out.shape[1]

    def fill(entry):
        first = entry_s[0, entry] * NH + count * step
        for index in range(count):
            row = beta[pl.ds(first + index, 1), :]
            phi_s[entry, 64 * index : 64 * index + 64] = (row * wave_s[...]).astype(BF16)

    fill(0)
    for entry in range(SPECIES + 1):
        if entry < SPECIES:
            fill(entry + 1)
        part = entry_s[1, entry]
        every = mm(phi_s[entry], site_s[part])
        members = kind_s[part, 0:1, :] == entry_s[0, entry].astype(F32)
        sum_s[part] = jnp.where(members, every, sum_s[part])

    for index in range(0, count, 2):
        for part in range(2):
            both = []
            for which in range(index, index + 2):
                real = sum_s[part, 64 * which : 64 * which + 32, :]
                imag = sum_s[part, 64 * which + 32 : 64 * which + 64, :]
                both.append(real[:, 0:half] - imag[:, half:])
                both.append(imag[:, 0:half] + real[:, half:])
            turned = jnp.concatenate(both, axis=0).T
            span = slice(part * half // 8, (part + 1) * half // 8)
            out[span, index // 2] = turned.reshape(half // 8, 8, 128)


def project(waves, beta, miller, kinds, sites):
    g_count = beta.shape[1]
    whole = lambda shape: pl.BlockSpec(shape, lambda i: (0,) * len(shape))
    return pl.pallas_call(
        project_kernel,
        grid=(HALF // PAIRS_A_STEP,),
        in_specs=[
            whole(waves.shape),
            whole(beta.shape),
            whole(miller.shape),
            whole((1, ATOMS)),
            whole(sites.shape),
        ],
        out_specs=pl.BlockSpec((ATOMS // 8, PAIRS_A_STEP, 8, 128), lambda i: (0, i, 0, 0)),
        out_shape=jax.ShapeDtypeStruct((ATOMS // 8, HALF, 8, 128), F32),
        scratch_shapes=[
            VMEM((2, 8, ATOMS), F32),
            VMEM((2, g_count, ATOMS), BF16),
            VMEM((64, g_count), F32),
            VMEM((SPECIES + 1, 128 * PAIRS_A_STEP, g_count), BF16),
            VMEM((2, 128 * PAIRS_A_STEP, ATOMS), F32),
            SMEM((2, SPECIES + 1), jnp.int32),
        ],
        name="project",
    )(waves, beta, miller, kinds.reshape(1, ATOMS), sites)


def pair_constants():
    ell = np.array([0, 0] + [1] * 6 + [2] * 10)
    first, second = np.triu_indices(NH)
    take = np.zeros((NH * 8, 256), np.float32)
    keep = np.zeros((NH, 256), np.float32)
    for p in range(PAIRS):
        take[second[p] * 8 : second[p] * 8 + 8, p] = 1.0
        keep[first[p], p] = 1.0 if first[p] == second[p] else 2.0
    lanes = np.zeros((8, 768), np.float32)
    lanes[:2] = -1.0
    for s in range(SPECIES):
        span = slice(s * PAIRS, (s + 1) * PAIRS)
        lanes[0, span] = np.arange(PAIRS)
        lanes[1, span] = s
        odd = (ell[first] + ell[second]) % 2
        lanes[2, span] = 1.0 - odd
        lanes[3, span] = -1.0 * odd
    return take, keep, lanes


def becsum_kernel(blocks, occ, take, keep, out):
    rows = []
    for pair in range(HALF):
        total = blocks[0, pair]
        for src in range(1, blocks.shape[0]):
            total = total + blocks[src, pair]
        if 1 <= pair <= 3:
            lane = iota((8, 128), 1)
            ahead = pltpu.roll(total, 96, 1)
            behind = pltpu.roll(total, 32, 1)
            total = jnp.where(lane % 64 < 32, -ahead, behind)
        elif pair >= 4:
            total = -total
        rows.append(total)
        rows.append(pltpu.roll(total, 64, 1))
    lane = iota((NH * 8, 128), 1)
    values = jnp.where(lane < 64, jnp.concatenate(rows, axis=0), 0.0)
    scaled = values * occ[...]
    square = lax.dot_general(
        scaled, values, (((1,), (1,)), ((), ())), precision=lax.Precision.HIGHEST,
        preferred_element_type=F32,
    )
    side = (NH * 8, NH * 8)
    square = jnp.where(iota(side, 0) % 8 == iota(side, 1) % 8, square, 0.0)
    high, low = split_two(square)
    lowest = (square - high.astype(F32) - low.astype(F32)).astype(BF16)
    chosen = mm(high, take[...]) + (mm(low, take[...]) + mm(lowest, take[...]))
    result = jnp.zeros((8, 256), F32)
    for i in range(NH):
        result = result + chosen[8 * i : 8 * i + 8] * keep[i : i + 1, :]
    tails = result[0:4, 128:256] + pltpu.roll(result[4:8, 128:256], 64, 1)
    packed = jnp.concatenate([result[0:4, 0:128], tails, result[4:8, 0:128]], axis=1)
    for peer in range(out.shape[0]):
        out[peer] = packed


def becsum_part(blocks, occupations, peers, take, keep):
    occ = jnp.tile(occupations, 4).reshape(1, 128)
    return pl.pallas_call(
        becsum_kernel,
        in_specs=resident(4),
        out_shape=jax.ShapeDtypeStruct((peers, 4, 384), F32),
        name="becsum",
        compiler_params=pltpu.CompilerParams(vmem_limit_bytes=12 * MIB),
    )(on_chip(blocks), on_chip(occ), on_chip(jnp.asarray(take, BF16)), on_chip(jnp.asarray(keep)))


def band_sum_kernel(parts, out):
    total = parts[0]
    for src in range(1, parts.shape[0]):
        total = total + parts[src]
    for peer in range(out.shape[0]):
        out[peer] = total


def band_sum(parts, peers):
    return pl.pallas_call(
        band_sum_kernel,
        in_specs=resident(1),
        out_shape=jax.ShapeDtypeStruct((peers, 4, 384), F32),
        name="band_sum",
        compiler_params=pltpu.CompilerParams(vmem_limit_bytes=8 * MIB),
    )(on_chip(parts))


def slot_column(sticks, slot):
    column = jnp.maximum(sticks[slot], 0)
    x_in_block = column // NY
    return x_in_block, column - x_in_block * NY


def structure_kernel(sticks, band, kinds, sites, out, kind_out, site_s):
    step = pl.program_id(0)
    chunk = out.shape[2]

    @pl.when(step == 0)
    def _():
        line = iota((ATOMS, ATOMS), 0)
        places = line % 128 // 4 * 8 + line // 128 * 4 + line % 4
        every, order = species_order(sites, kinds, places)
        columns = mm_nt(order, every)
        for d in range(3):
            site_s[d] = jnp.broadcast_to(columns[:, d : d + 1], (ATOMS, 128))
        kind_out[...] = jnp.broadcast_to(columns[:, 3:4], (ATOMS, 128))

    g_row = step * chunk + iota((1, chunk), 1)
    slot_row = jnp.zeros((1, chunk), jnp.int32)
    for slot in range(1, 8):
        slot_row = slot_row + (g_row >= slot * NZ).astype(jnp.int32)
    z_row = (g_row - slot_row * NZ).astype(F32)
    x_row = jnp.zeros((1, chunk), F32)
    y_row = jnp.zeros((1, chunk), F32)
    live_row = jnp.zeros((1, chunk), F32)
    for slot in range(8):
        x_in_block, y_value = slot_column(sticks, slot)
        x_value = band[0] * (NX // 16) + x_in_block
        here = slot_row == slot
        x_row = jnp.where(here, x_value.astype(F32), x_row)
        y_row = jnp.where(here, y_value.astype(F32), y_row)
        live_row = jnp.where(here, (sticks[slot] >= 0).astype(F32), live_row)
    reps = chunk // 128
    site_cols = [jnp.concatenate([site_s[d]] * reps, axis=1) for d in range(3)]
    cosine, sine = site_waves(site_cols, [x_row, y_row, z_row])
    out[0] = cosine * live_row
    out[1] = sine * live_row


def structure(sticks, band, kinds, sites, count):
    chunk = 256
    whole = lambda shape: pl.BlockSpec(shape, lambda i: (0,) * len(shape))
    scalar = pl.BlockSpec(memory_space=SMEM)
    return pl.pallas_call(
        structure_kernel,
        grid=(count // chunk,),
        in_specs=[scalar, scalar, whole((1, ATOMS)), whole(sites.shape)],
        out_specs=[
            pl.BlockSpec((2, ATOMS, chunk), lambda i: (0, 0, i)),
            pl.BlockSpec(memory_space=VMEM),
        ],
        out_shape=[
            jax.ShapeDtypeStruct((2, ATOMS, count), F32),
            VMEM((ATOMS, 128), F32),
        ],
        scratch_shapes=[VMEM((3, ATOMS, 128), F32)],
        cost_estimate=pl.CostEstimate(flops=60 * ATOMS * count, transcendentals=0, bytes_accessed=8 * ATOMS * count),
        name="structure",
    )(sticks, band, kinds.reshape(1, ATOMS), sites)


def augment_kernel(
    sticks, becsum, kinds, lanes, cos_high, cos_low, sin_high, sin_low, phases_far,
    table_far, out, aug_s, phases, table, sems,
):
    copies = []
    for index in range(table.shape[1] // 256):
        span = pl.ds(index * 256, 256)
        copies.append(
            [
                pltpu.make_async_copy(table_far.at[:, span], table.at[:, span], sems.at[0, index]),
                pltpu.make_async_copy(
                    phases_far.at[:, :, span], phases.at[:, :, span], sems.at[1, index]
                ),
            ]
        )
    for needed in copies[0:AHEAD]:
        for copy in needed:
            copy.start()
    width = lanes.shape[1]
    spread = (iota((256, width), 0).astype(F32) == lanes[0:1, :]).astype(F32).astype(BF16)
    packed = becsum[...].reshape(128, 384)
    tail = packed[:, 128:256]
    rounded = jnp.concatenate(
        [
            jnp.concatenate([packed[:, 0:128], tail], axis=1),
            jnp.concatenate([packed[:, 256:384], pltpu.roll(tail, 64, 1)], axis=1),
        ],
        axis=0,
    ).astype(BF16)
    mine = jnp.where(kinds[:, 0:1] == lanes[1:2, :], mm(rounded, spread), 0.0)
    rows = table.shape[0]
    even = (mine * lanes[2:3, :]).astype(BF16)[:, 0:rows]
    odd = (mine * lanes[3:4, :]).astype(BF16)[:, 0:rows]
    for start in range(0, table.shape[1], 256):
        span = slice(start, start + 256)
        if start // 256 + AHEAD < len(copies):
            for copy in copies[start // 256 + AHEAD]:
                copy.start()
        for copy in copies[start // 256]:
            copy.wait()
        amp_re = mm(even, table[:, span])
        amp_im = mm(odd, table[:, span])
        cosine = phases[0, :, span]
        sine = phases[1, :, span]
        aug_s[0:1, span] = jnp.sum(amp_re * cosine + amp_im * sine, axis=0, keepdims=True)
        aug_s[1:2, span] = jnp.sum(amp_im * cosine - amp_re * sine, axis=0, keepdims=True)
    stick = [aug_s[0:1, s * NZ : (s + 1) * NZ] for s in range(8)]
    stick += [aug_s[1:2, s * NZ : (s + 1) * NZ] for s in range(8)]
    data = jnp.concatenate(stick, axis=0)
    by_cos = mm_three(data, cos_high[...], cos_low[...])
    by_sin = mm_three(data, sin_high[...], sin_low[...])
    out_re = by_cos[0:8] - by_sin[8:16]
    out_im = by_sin[0:8] + by_cos[8:16]
    sub = iota((8, 256), 0)
    x_info = jnp.zeros((8, 256), F32)
    y_info = jnp.zeros((8, 256), F32)
    for slot in range(8):
        x_in_block, y_value = slot_column(sticks, slot)
        x_info = jnp.where(sub == slot, x_in_block.astype(F32), x_info)
        y_info = jnp.where(sub == slot, y_value.astype(F32), y_info)
    lane = iota((8, 256), 1)
    out_re = jnp.where(lane < NZ, out_re, x_info)
    out_im = jnp.where(lane < NZ, out_im, y_info)
    turned = jnp.concatenate([out_re, out_im], axis=0).T
    out[...] = jnp.concatenate([turned[32 * j : 32 * j + 32] for j in range(8)], axis=1)


def z_tables():
    z = np.arange(NZ)
    plane = np.zeros(256, np.int64)
    plane[:NZ] = 7 * (np.arange(NZ) % 32) + np.arange(NZ) // 32
    angle = 2 * np.pi * ((z[:, None] * plane[None, :]) % NZ) / NZ
    live = (np.arange(256) < NZ)[None, :]
    return np.cos(angle) * live, np.sin(angle) * live


def halves(table):
    table = np.asarray(table, np.float32)
    high = table.astype(jnp.bfloat16)
    return jnp.asarray(high), jnp.asarray((table - high.astype(np.float32)).astype(jnp.bfloat16))


def augment(sticks, becsum, kinds, phases, lanes, table):
    cosine, sine = z_tables()
    constants = [on_chip(c) for c in (*halves(cosine), *halves(sine))]
    return pl.pallas_call(
        augment_kernel,
        in_specs=[pl.BlockSpec(memory_space=SMEM)]
        + resident(7)
        + [pl.BlockSpec(memory_space=pltpu.HBM)] * 2,
        out_shape=jax.ShapeDtypeStruct((32, 128), F32),
        scratch_shapes=[
            VMEM((8, table.shape[1]), F32),
            VMEM(phases.shape, F32),
            VMEM(table.shape, BF16),
            pltpu.SemaphoreType.DMA((2, table.shape[1] // 256)),
        ],
        name="augment",
    )(
        sticks, on_chip(becsum), on_chip(kinds), on_chip(jnp.asarray(lanes)), *constants, phases,
        table,
    )


def spread_constants():
    spread = np.zeros((8, 128, 256), np.float32)
    for slot in range(8):
        for j in range(8):
            for part in range(2):
                row = j * 16 + part * 8 + slot
                spread[slot, row, part * 128 + j * 16 : part * 128 + j * 16 + 16] = 1.0
    return spread


def y_kernel(values, spread, out):
    high, low = split_two(values[...].reshape(32, 128))
    parts = []
    for slot in range(8):
        parts.append(mm(high, spread[slot]) + mm(low, spread[slot]))
    wide = jnp.concatenate(parts, axis=0)
    y_col = wide[:, 240:241]
    source = jnp.where(iota((8, 256), 0) == 0, 112, 240)
    pick = (iota((8, 256), 1) == source).astype(F32).astype(BF16)
    info = mm_nt(pick, wide.astype(BF16))
    x_t = info[0:1, :]
    y_t = info[1:2, :]
    lane = iota((256, 128), 1)
    cosine, sine = turn_waves(turns_of(y_col * (lane % 16).astype(F32), NY))
    real = wide[:, 0:128]
    imag = wide[:, 128:256]
    keep = lane < 112
    new_re = jnp.where(keep, real * cosine - imag * sine, 0.0)
    new_im = jnp.where(keep, real * sine + imag * cosine, 0.0)
    right = jnp.concatenate(
        [
            jnp.concatenate([new_re, new_im], axis=1),
            jnp.concatenate([-new_im, new_re], axis=1),
        ],
        axis=0,
    )
    line = iota((256, 256), 0)
    here = (line % 16).astype(F32) == x_t
    far_cos, far_sin = turn_waves(turns_of(y_t * (line // 16).astype(F32), 16))
    left = jnp.concatenate([jnp.where(here, far_cos, 0.0), jnp.where(here, far_sin, 0.0)], axis=1)
    right_high, right_low = split_two(right)
    out[...] = mm_three(left, right_high, right_low).reshape(16, 16, 256)


def y_transform(values):
    spread = jnp.asarray(spread_constants(), BF16)
    return pl.pallas_call(
        y_kernel,
        in_specs=resident(2),
        out_shape=jax.ShapeDtypeStruct((16, 16, 256), F32),
        name="y_transform",
        compiler_params=pltpu.CompilerParams(vmem_limit_bytes=12 * MIB),
    )(on_chip(values), on_chip(spread))


def x_tables():
    row = np.arange(256)
    x_in = 15 * (row // 16) + row % 16
    x_out = np.arange(256)
    angle = 2 * np.pi * ((x_in[:, None] * x_out[None, :]) % NX) / NX
    live = (row % 16 < 15)[:, None] & (x_out < NX)[None, :]
    return np.cos(angle) * live, np.sin(angle) * live


def x_kernel(values, cos_high, cos_low, sin_high, sin_low, out):
    turned = values[...].reshape(256, 256).T
    by_cos = mm_three(turned, cos_high[...], cos_low[...])
    by_sin = mm_three(turned, sin_high[...], sin_low[...])
    real = by_cos[0:128] - by_sin[128:256]
    imag = by_sin[0:128] + by_cos[128:256]
    for j in range(7):
        out[j, :, 0, :] = real[16 * j : 16 * j + 15, 0:NX]
        out[j, :, 1, :] = imag[16 * j : 16 * j + 15, 0:NX]


def x_transform(values):
    cosine, sine = x_tables()
    constants = [on_chip(c) for c in (*halves(cosine), *halves(sine))]
    result = pl.pallas_call(
        x_kernel,
        in_specs=resident(5),
        out_shape=jax.ShapeDtypeStruct((7, 15, 2, NX), F32),
        name="x_transform",
        compiler_params=pltpu.CompilerParams(vmem_limit_bytes=12 * MIB),
    )(on_chip(values), *constants)
    return jnp.transpose(result, (2, 0, 1, 3))


def on_chip(value):
    return pltpu.with_memory_space_constraint(value, VMEM)


def resident(count):
    return [pl.BlockSpec(memory_space=VMEM)] * count


def exchange(value, axis):
    return lax.all_to_all(value, axis, 0, 0, tiled=True)


def on_device(
    waves, occupations, beta_table, wave_miller, atom_kinds, atom_sites, aug_table, stick_columns
):
    take, keep, lanes = pair_constants()
    bands = lax.axis_size("band")
    groups = lax.axis_size("ga")
    band = lax.axis_index("band").reshape(1)
    pieces = project(waves, beta_table, wave_miller, atom_kinds, atom_sites)
    phases, kind_columns = structure(
        stick_columns, band, atom_kinds, atom_sites, aug_table.shape[1]
    )
    occupations, phases = lax.optimization_barrier((occupations, phases))
    pieces = exchange(pieces, "ga")
    part = becsum_part(pieces, occupations, bands, take, keep)
    summed = band_sum(exchange(part, "band"), groups)
    becsum = exchange(summed, "ga")
    columns = augment(stick_columns, becsum, kind_columns, phases, lanes, aug_table)
    planes = y_transform(exchange(columns.reshape(32, 1, 128), "ga"))
    return x_transform(exchange(planes, "band"))


def solution(mesh):
    in_specs = (
        P(None, "band", "ga"),
        P("band"),
        P(None, "ga"),
        P(None, "ga"),
        P(),
        P(),
        P(None, ("band", "ga")),
        P(("band", "ga")),
    )
    out_specs = P(None, "ga", "band", None)
    return jax.shard_map(
        on_device, mesh=mesh, in_specs=in_specs, out_specs=out_specs, check_vma=False
    )
```

```python
import math

import jax
import jax.numpy as jnp
import numpy as np
from jax import lax
from jax.experimental import pallas as pl
from jax.experimental.pallas import tpu as pltpu
from jax.sharding import PartitionSpec as P

NX = 240
NY = 240
NZ = 224
NH = 18
PAIRS = 171
SPECIES = 4
ATOMS = 256
HALF = NH // 2
PAIRS_A_STEP = 3
F32 = jnp.float32
BF16 = jnp.bfloat16
VMEM = pltpu.VMEM
SMEM = pltpu.SMEM
MIB = 1 << 20
NEAR = 2


def turn_polynomials():
    nodes = np.cos(np.pi * (np.arange(400) + 0.5) / 400)
    squares = 0.125 + 0.125 * nodes
    turns = np.sqrt(squares)
    sine = np.polynomial.chebyshev.Chebyshev.fit(
        squares, np.sin(2 * np.pi * turns) / turns, 6, domain=[0, 0.25]
    )
    cosine = np.polynomial.chebyshev.Chebyshev.fit(
        squares, np.cos(2 * np.pi * turns), 6, domain=[0, 0.25]
    )
    poly = np.polynomial.polynomial.Polynomial
    return (
        [float(v) for v in sine.convert(kind=poly).coef],
        [float(v) for v in cosine.convert(kind=poly).coef],
    )


SINE_TERMS, COSINE_TERMS = turn_polynomials()


def horner(terms, value):
    total = jnp.full_like(value, terms[-1])
    for term in terms[-2::-1]:
        total = total * value + term
    return total


def turn_waves(turns):
    square = turns * turns
    return horner(COSINE_TERMS, square), turns * horner(SINE_TERMS, square)


def turns_of(count, length):
    return (count - length * jnp.round(count * (1.0 / length))) * (1.0 / length)


def site_waves(site_cols, miller_rows):
    parts = math.lcm(NX, NY, NZ)
    rows = [row * (parts // length) for row, length in zip(miller_rows, (NX, NY, NZ))]
    count = site_cols[0] * rows[0] + site_cols[1] * rows[1] + site_cols[2] * rows[2]
    return turn_waves(turns_of(count, parts))


def iota(shape, dim):
    return lax.broadcasted_iota(jnp.int32, shape, dim)


def split_two(value):
    high = value.astype(BF16)
    return high, (value - high.astype(F32)).astype(BF16)


def mm(left, right):
    return jnp.dot(left, right, preferred_element_type=F32)


def mm_nt(left, right):
    return lax.dot_general(left, right, (((1,), (1,)), ((), ())), preferred_element_type=F32)


def mm_three(left, right_high, right_low):
    high, low = split_two(left)
    return mm(high, right_high) + (mm(high, right_low) + mm(low, right_high))


def as_columns(rows):
    eye = (iota((ATOMS, ATOMS), 0) == iota((ATOMS, ATOMS), 1)).astype(F32).astype(BF16)
    return mm_nt(eye, rows.astype(BF16))


def species_order(sites, kinds, places):
    kind_row = kinds[...].astype(F32)
    every = [sites[...].astype(F32), kind_row, jnp.zeros((4, ATOMS), F32)]
    every = jnp.concatenate(every, axis=0).astype(BF16)
    eye = (iota((ATOMS, ATOMS), 0) == iota((ATOMS, ATOMS), 1)).astype(F32).astype(BF16)
    kind_col = mm_nt(eye, every)[:, 3:4]
    earlier = iota((ATOMS, ATOMS), 0) < iota((ATOMS, ATOMS), 1)
    ahead = (kind_col < kind_row) | ((kind_col == kind_row) & earlier)
    rank = jnp.sum(ahead.astype(F32), axis=0, keepdims=True)
    return every, (places.astype(F32) == rank).astype(F32).astype(BF16)


def project_kernel(
    waves_far, beta_far, miller, kinds, sites, out, kind_s, site_s, wave_s, phi_s, sum_s, entry_s,
    waves, beta, sems,
):
    g_count = beta.shape[1]
    half = ATOMS // 2
    step = pl.program_id(0)
    loads = [
        pltpu.make_async_copy(waves_far, waves, sems.at[0]),
        pltpu.make_async_copy(beta_far, beta, sems.at[1]),
    ]

    @pl.when(step == 0)
    def _():
        for load in loads:
            load.start()
        below = jnp.int32(0)
        last = jnp.int32(0)
        for species in range(SPECIES - 1):
            below = below + jnp.sum((kinds[...] == species).astype(jnp.int32))
            last = last + (below < half).astype(jnp.int32)
        for entry in range(SPECIES + 1):
            later = (entry > last).astype(jnp.int32)
            entry_s[0, entry] = entry - later
            entry_s[1, entry] = later
        every, order = species_order(sites, kinds, iota((ATOMS, ATOMS), 0))
        mine = mm_nt(every, order)
        for part in range(2):
            span = slice(part * half, part * half + half)
            kind_s[part, 0:1, 0:half] = mine[3:4, span]
            kind_s[part, 0:1, half:] = mine[3:4, span]
        site_rows = [mine[d : d + 1] for d in range(3)]
        for start in range(0, g_count, 256):
            rows = [miller[:, start : start + 256].astype(F32), jnp.zeros((5, 256), F32)]
            columns = as_columns(jnp.concatenate(rows, axis=0))
            cosine, sine = site_waves([columns[:, d : d + 1] for d in range(3)], site_rows)
            for part in range(2):
                span = slice(part * half, part * half + half)
                site_s[part, start : start + 256, 0:half] = cosine[:, span].astype(BF16)
                site_s[part, start : start + 256, half:] = sine[:, span].astype(BF16)
        for load in loads:
            load.wait()
        wave_s[0:32] = waves[0].astype(F32)
        wave_s[32:64] = waves[1].astype(F32)

    count = 2 * out.shape[1]

    def fill(entry):
        first = entry_s[0, entry] * NH + count * step
        for index in range(count):
            row = beta[pl.ds(first + index, 1), :]
            phi_s[entry, 64 * index : 64 * index + 64] = (row * wave_s[...]).astype(BF16)

    fill(0)
    for entry in range(SPECIES + 1):
        if entry < SPECIES:
            fill(entry + 1)
        part = entry_s[1, entry]
        every = mm(phi_s[entry], site_s[part])
        members = kind_s[part, 0:1, :] == entry_s[0, entry].astype(F32)
        sum_s[part] = jnp.where(members, every, sum_s[part])

    for index in range(0, count, 2):
        for part in range(2):
            both = []
            for which in range(index, index + 2):
                real = sum_s[part, 64 * which : 64 * which + 32, :]
                imag = sum_s[part, 64 * which + 32 : 64 * which + 64, :]
                both.append(real[:, 0:half] - imag[:, half:])
                both.append(imag[:, 0:half] + real[:, half:])
            turned = jnp.concatenate(both, axis=0).T
            span = slice(part * half // 8, (part + 1) * half // 8)
            out[span, index // 2] = turned.reshape(half // 8, 8, 128)


def project(waves, beta, miller, kinds, sites):
    g_count = beta.shape[1]
    whole = lambda shape: pl.BlockSpec(shape, lambda i: (0,) * len(shape))
    return pl.pallas_call(
        project_kernel,
        grid=(HALF // PAIRS_A_STEP,),
        in_specs=[
            pl.BlockSpec(memory_space=pltpu.HBM),
            pl.BlockSpec(memory_space=pltpu.HBM),
            whole(miller.shape),
            whole((1, ATOMS)),
            whole(sites.shape),
        ],
        out_specs=pl.BlockSpec((ATOMS // 8, PAIRS_A_STEP, 8, 128), lambda i: (0, i, 0, 0)),
        out_shape=jax.ShapeDtypeStruct((ATOMS // 8, HALF, 8, 128), F32),
        scratch_shapes=[
            VMEM((2, 8, ATOMS), F32),
            VMEM((2, g_count, ATOMS), BF16),
            VMEM((64, g_count), F32),
            VMEM((SPECIES + 1, 128 * PAIRS_A_STEP, g_count), BF16),
            VMEM((2, 128 * PAIRS_A_STEP, ATOMS), F32),
            SMEM((2, SPECIES + 1), jnp.int32),
            VMEM(waves.shape, BF16),
            VMEM(beta.shape, F32),
            pltpu.SemaphoreType.DMA((2,)),
        ],
        name="project",
    )(waves, beta, miller, kinds.reshape(1, ATOMS), sites)


def pair_constants():
    ell = np.array([0, 0] + [1] * 6 + [2] * 10)
    first, second = np.triu_indices(NH)
    take = np.zeros((NH * 8, 256), np.float32)
    keep = np.zeros((NH, 256), np.float32)
    for p in range(PAIRS):
        take[second[p] * 8 : second[p] * 8 + 8, p] = 1.0
        keep[first[p], p] = 1.0 if first[p] == second[p] else 2.0
    lanes = np.zeros((8, 768), np.float32)
    lanes[:2] = -1.0
    for s in range(SPECIES):
        span = slice(s * PAIRS, (s + 1) * PAIRS)
        lanes[0, span] = np.arange(PAIRS)
        lanes[1, span] = s
        odd = (ell[first] + ell[second]) % 2
        lanes[2, span] = 1.0 - odd
        lanes[3, span] = -1.0 * odd
    return take, keep, lanes


def becsum_kernel(blocks, occ, take, keep, out):
    rows = []
    for pair in range(HALF):
        total = blocks[0, pair]
        for src in range(1, blocks.shape[0]):
            total = total + blocks[src, pair]
        if 1 <= pair <= 3:
            lane = iota((8, 128), 1)
            ahead = pltpu.roll(total, 96, 1)
            behind = pltpu.roll(total, 32, 1)
            total = jnp.where(lane % 64 < 32, -ahead, behind)
        elif pair >= 4:
            total = -total
        rows.append(total)
        rows.append(pltpu.roll(total, 64, 1))
    lane = iota((NH * 8, 128), 1)
    values = jnp.where(lane < 64, jnp.concatenate(rows, axis=0), 0.0)
    scaled = values * occ[...]
    square = lax.dot_general(
        scaled, values, (((1,), (1,)), ((), ())), precision=lax.Precision.HIGHEST,
        preferred_element_type=F32,
    )
    side = (NH * 8, NH * 8)
    square = jnp.where(iota(side, 0) % 8 == iota(side, 1) % 8, square, 0.0)
    high, low = split_two(square)
    lowest = (square - high.astype(F32) - low.astype(F32)).astype(BF16)
    chosen = mm(high, take[...]) + (mm(low, take[...]) + mm(lowest, take[...]))
    result = jnp.zeros((8, 256), F32)
    for i in range(NH):
        result = result + chosen[8 * i : 8 * i + 8] * keep[i : i + 1, :]
    tails = result[0:4, 128:256] + pltpu.roll(result[4:8, 128:256], 64, 1)
    packed = jnp.concatenate([result[0:4, 0:128], tails, result[4:8, 0:128]], axis=1)
    for peer in range(out.shape[0]):
        out[peer] = packed


def becsum_part(blocks, occupations, peers, take, keep):
    occ = jnp.tile(occupations, 4).reshape(1, 128)
    return pl.pallas_call(
        becsum_kernel,
        in_specs=resident(4),
        out_shape=jax.ShapeDtypeStruct((peers, 4, 384), F32),
        name="becsum",
        compiler_params=pltpu.CompilerParams(vmem_limit_bytes=12 * MIB),
    )(on_chip(blocks), on_chip(occ), on_chip(jnp.asarray(take, BF16)), on_chip(jnp.asarray(keep)))


def band_sum_kernel(parts, out):
    total = parts[0]
    for src in range(1, parts.shape[0]):
        total = total + parts[src]
    for peer in range(out.shape[0]):
        out[peer] = total


def band_sum(parts, peers):
    return pl.pallas_call(
        band_sum_kernel,
        in_specs=resident(1),
        out_shape=jax.ShapeDtypeStruct((peers, 4, 384), F32),
        name="band_sum",
        compiler_params=pltpu.CompilerParams(vmem_limit_bytes=8 * MIB),
    )(on_chip(parts))


def slot_column(sticks, slot):
    column = jnp.maximum(sticks[slot], 0)
    x_in_block = column // NY
    return x_in_block, column - x_in_block * NY


def column_waves(sticks, band, site_cols, first, chunk):
    g_row = first + iota((1, chunk), 1)
    slot_row = jnp.zeros((1, chunk), jnp.int32)
    for slot in range(1, 8):
        slot_row = slot_row + (g_row >= slot * NZ).astype(jnp.int32)
    z_row = (g_row - slot_row * NZ).astype(F32)
    x_row = jnp.zeros((1, chunk), F32)
    y_row = jnp.zeros((1, chunk), F32)
    live_row = jnp.zeros((1, chunk), F32)
    for slot in range(8):
        x_in_block, y_value = slot_column(sticks, slot)
        x_value = band[0] * (NX // 16) + x_in_block
        here = slot_row == slot
        x_row = jnp.where(here, x_value.astype(F32), x_row)
        y_row = jnp.where(here, y_value.astype(F32), y_row)
        live_row = jnp.where(here, (sticks[slot] >= 0).astype(F32), live_row)
    cosine, sine = site_waves(site_cols, [x_row, y_row, z_row])
    return cosine * live_row, sine * live_row


def structure_kernel(sticks, band, kinds, sites, out, atoms_out, site_s):
    step = pl.program_id(0)
    chunk = out.shape[2]

    @pl.when(step == 0)
    def _():
        line = iota((ATOMS, ATOMS), 0)
        places = line % 128 // 4 * 8 + line // 128 * 4 + line % 4
        every, order = species_order(sites, kinds, places)
        columns = mm_nt(order, every)
        for d in range(3):
            site_s[d] = jnp.broadcast_to(columns[:, d : d + 1], (ATOMS, chunk))
        atoms_out[...] = jnp.concatenate([columns, jnp.zeros((ATOMS, 120), F32)], axis=1)

    site_cols = [site_s[d] for d in range(3)]
    cosine, sine = column_waves(sticks, band, site_cols, (step + NEAR) * chunk, chunk)
    out[0] = cosine
    out[1] = sine


def structure(sticks, band, kinds, sites, count):
    chunk = 256
    count = count - NEAR * chunk
    whole = lambda shape: pl.BlockSpec(shape, lambda i: (0,) * len(shape))
    scalar = pl.BlockSpec(memory_space=SMEM)
    return pl.pallas_call(
        structure_kernel,
        grid=(count // chunk,),
        in_specs=[scalar, scalar, whole((1, ATOMS)), whole(sites.shape)],
        out_specs=[
            pl.BlockSpec((2, ATOMS, chunk), lambda i: (0, 0, i)),
            pl.BlockSpec(memory_space=VMEM),
        ],
        out_shape=[
            jax.ShapeDtypeStruct((2, ATOMS, count), F32),
            VMEM((ATOMS, 128), F32),
        ],
        scratch_shapes=[VMEM((3, ATOMS, chunk), F32)],
        cost_estimate=pl.CostEstimate(
            flops=60 * ATOMS * count, transcendentals=0, bytes_accessed=8 * ATOMS * count
        ),
        name="structure",
    )(sticks, band, kinds.reshape(1, ATOMS), sites)


def augment_kernel(
    sticks, band, becsum, atoms, lanes, cos_high, cos_low, sin_high, sin_low, phases_far,
    table_far, out, aug_s, phases, table, sems,
):
    copies = []
    for index in range(table.shape[1] // 256):
        span = pl.ds(index * 256, 256)
        needed = [
            pltpu.make_async_copy(table_far.at[:, span], table.at[:, span], sems.at[0, index])
        ]
        if index >= NEAR:
            here = pl.ds((index - NEAR) * 256, 256)
            needed.append(
                pltpu.make_async_copy(phases_far.at[:, :, here], phases.at[:, :, span], sems.at[1, index])
            )
        for copy in needed:
            copy.start()
        copies.append(needed)
    site_cols = [jnp.broadcast_to(atoms[:, d : d + 1], (ATOMS, 256)) for d in range(3)]
    for start in range(0, NEAR * 256, 256):
        cosine, sine = column_waves(sticks, band, site_cols, start, 256)
        phases[0, :, start : start + 256] = cosine
        phases[1, :, start : start + 256] = sine
    width = lanes.shape[1]
    spread = (iota((256, width), 0).astype(F32) == lanes[0:1, :]).astype(F32).astype(BF16)
    packed = becsum[...].reshape(128, 384)
    tail = packed[:, 128:256]
    rounded = jnp.concatenate(
        [
            jnp.concatenate([packed[:, 0:128], tail], axis=1),
            jnp.concatenate([packed[:, 256:384], pltpu.roll(tail, 64, 1)], axis=1),
        ],
        axis=0,
    ).astype(BF16)
    mine = jnp.where(atoms[:, 3:4] == lanes[1:2, :], mm(rounded, spread), 0.0)
    rows = table.shape[0]
    even = (mine * lanes[2:3, :]).astype(BF16)[:, 0:rows]
    odd = (mine * lanes[3:4, :]).astype(BF16)[:, 0:rows]
    for start in range(0, table.shape[1], 256):
        span = slice(start, start + 256)
        for copy in copies[start // 256]:
            copy.wait()
        amp_re = mm(even, table[:, span])
        amp_im = mm(odd, table[:, span])
        cosine = phases[0, :, span]
        sine = phases[1, :, span]
        aug_s[0:1, span] = jnp.sum(amp_re * cosine + amp_im * sine, axis=0, keepdims=True)
        aug_s[1:2, span] = jnp.sum(amp_im * cosine - amp_re * sine, axis=0, keepdims=True)
    stick = [aug_s[0:1, s * NZ : (s + 1) * NZ] for s in range(8)]
    stick += [aug_s[1:2, s * NZ : (s + 1) * NZ] for s in range(8)]
    data = jnp.concatenate(stick, axis=0)
    by_cos = mm_three(data, cos_high[...], cos_low[...])
    by_sin = mm_three(data, sin_high[...], sin_low[...])
    out_re = by_cos[0:8] - by_sin[8:16]
    out_im = by_sin[0:8] + by_cos[8:16]
    sub = iota((8, 256), 0)
    x_info = jnp.zeros((8, 256), F32)
    y_info = jnp.zeros((8, 256), F32)
    for slot in range(8):
        x_in_block, y_value = slot_column(sticks, slot)
        x_info = jnp.where(sub == slot, x_in_block.astype(F32), x_info)
        y_info = jnp.where(sub == slot, y_value.astype(F32), y_info)
    lane = iota((8, 256), 1)
    out_re = jnp.where(lane < NZ, out_re, x_info)
    out_im = jnp.where(lane < NZ, out_im, y_info)
    turned = jnp.concatenate([out_re, out_im], axis=0).T
    out[...] = jnp.concatenate([turned[32 * j : 32 * j + 32] for j in range(8)], axis=1)


def z_tables():
    z = np.arange(NZ)
    plane = np.zeros(256, np.int64)
    plane[:NZ] = 7 * (np.arange(NZ) % 32) + np.arange(NZ) // 32
    angle = 2 * np.pi * ((z[:, None] * plane[None, :]) % NZ) / NZ
    live = (np.arange(256) < NZ)[None, :]
    return np.cos(angle) * live, np.sin(angle) * live


def halves(table):
    table = np.asarray(table, np.float32)
    high = table.astype(jnp.bfloat16)
    return jnp.asarray(high), jnp.asarray((table - high.astype(np.float32)).astype(jnp.bfloat16))


def augment(sticks, band, becsum, atoms, phases, lanes, table):
    cosine, sine = z_tables()
    constants = [on_chip(c) for c in (*halves(cosine), *halves(sine))]
    return pl.pallas_call(
        augment_kernel,
        in_specs=[pl.BlockSpec(memory_space=SMEM)] * 2
        + resident(7)
        + [pl.BlockSpec(memory_space=pltpu.HBM)] * 2,
        out_shape=jax.ShapeDtypeStruct((32, 128), F32),
        scratch_shapes=[
            VMEM((8, table.shape[1]), F32),
            VMEM((2, ATOMS, table.shape[1]), F32),
            VMEM(table.shape, BF16),
            pltpu.SemaphoreType.DMA((2, table.shape[1] // 256)),
        ],
        name="augment",
    )(
        sticks, band, on_chip(becsum), on_chip(atoms), on_chip(jnp.asarray(lanes)), *constants, phases,
        table,
    )


def spread_constants():
    spread = np.zeros((8, 128, 256), np.float32)
    for slot in range(8):
        for j in range(8):
            for part in range(2):
                row = j * 16 + part * 8 + slot
                spread[slot, row, part * 128 + j * 16 : part * 128 + j * 16 + 16] = 1.0
    return spread


def y_kernel(values, spread, out):
    high, low = split_two(values[...].reshape(32, 128))
    parts = []
    for slot in range(8):
        parts.append(mm(high, spread[slot]) + mm(low, spread[slot]))
    wide = jnp.concatenate(parts, axis=0)
    y_col = wide[:, 240:241]
    source = jnp.where(iota((8, 256), 0) == 0, 112, 240)
    pick = (iota((8, 256), 1) == source).astype(F32).astype(BF16)
    info = mm_nt(pick, wide.astype(BF16))
    x_t = info[0:1, :]
    y_t = info[1:2, :]
    lane = iota((256, 128), 1)
    cosine, sine = turn_waves(turns_of(y_col * (lane % 16).astype(F32), NY))
    real = wide[:, 0:128]
    imag = wide[:, 128:256]
    keep = lane < 112
    new_re = jnp.where(keep, real * cosine - imag * sine, 0.0)
    new_im = jnp.where(keep, real * sine + imag * cosine, 0.0)
    right = jnp.concatenate(
        [
            jnp.concatenate([new_re, new_im], axis=1),
            jnp.concatenate([-new_im, new_re], axis=1),
        ],
        axis=0,
    )
    line = iota((256, 256), 0)
    here = (line % 16).astype(F32) == x_t
    far_cos, far_sin = turn_waves(turns_of(y_t * (line // 16).astype(F32), 16))
    left = jnp.concatenate([jnp.where(here, far_cos, 0.0), jnp.where(here, far_sin, 0.0)], axis=1)
    right_high, right_low = split_two(right)
    out[...] = mm_three(left, right_high, right_low).reshape(16, 16, 256)


def y_transform(values):
    spread = jnp.asarray(spread_constants(), BF16)
    return pl.pallas_call(
        y_kernel,
        in_specs=resident(2),
        out_shape=jax.ShapeDtypeStruct((16, 16, 256), F32),
        name="y_transform",
        compiler_params=pltpu.CompilerParams(vmem_limit_bytes=12 * MIB),
    )(on_chip(values), on_chip(spread))


def x_tables():
    row = np.arange(256)
    x_in = 15 * (row // 16) + row % 16
    x_out = np.arange(256)
    angle = 2 * np.pi * ((x_in[:, None] * x_out[None, :]) % NX) / NX
    live = (row % 16 < 15)[:, None] & (x_out < NX)[None, :]
    return np.cos(angle) * live, np.sin(angle) * live


def x_kernel(values, cos_high, cos_low, sin_high, sin_low, out):
    turned = values[...].reshape(256, 256).T
    by_cos = mm_three(turned, cos_high[...], cos_low[...])
    by_sin = mm_three(turned, sin_high[...], sin_low[...])
    real = by_cos[0:128] - by_sin[128:256]
    imag = by_sin[0:128] + by_cos[128:256]
    for j in range(7):
        out[j, :, 0, :] = real[16 * j : 16 * j + 15, 0:NX]
        out[j, :, 1, :] = imag[16 * j : 16 * j + 15, 0:NX]


def x_transform(values):
    cosine, sine = x_tables()
    constants = [on_chip(c) for c in (*halves(cosine), *halves(sine))]
    result = pl.pallas_call(
        x_kernel,
        in_specs=resident(5),
        out_shape=jax.ShapeDtypeStruct((7, 15, 2, NX), F32),
        name="x_transform",
        compiler_params=pltpu.CompilerParams(vmem_limit_bytes=12 * MIB),
    )(on_chip(values), *constants)
    return jnp.transpose(result, (2, 0, 1, 3))


def on_chip(value):
    return pltpu.with_memory_space_constraint(value, VMEM)


def resident(count):
    return [pl.BlockSpec(memory_space=VMEM)] * count


def exchange(value, axis):
    return lax.all_to_all(value, axis, 0, 0, tiled=True)


def on_device(
    waves, occupations, beta_table, wave_miller, atom_kinds, atom_sites, aug_table, stick_columns
):
    take, keep, lanes = pair_constants()
    bands = lax.axis_size("band")
    groups = lax.axis_size("ga")
    band = lax.axis_index("band").reshape(1)
    pieces = project(waves, beta_table, wave_miller, atom_kinds, atom_sites)
    phases, atoms = structure(
        stick_columns, band, atom_kinds, atom_sites, aug_table.shape[1]
    )
    occupations, phases = lax.optimization_barrier((occupations, phases))
    pieces = exchange(pieces, "ga")
    part = becsum_part(pieces, occupations, bands, take, keep)
    summed = band_sum(exchange(part, "band"), groups)
    becsum = exchange(summed, "ga")
    columns = augment(stick_columns, band, becsum, atoms, phases, lanes, aug_table)
    planes = y_transform(exchange(columns.reshape(32, 1, 128), "ga"))
    return x_transform(exchange(planes, "band"))


def solution(mesh):
    in_specs = (
        P(None, "band", "ga"),
        P("band"),
        P(None, "ga"),
        P(None, "ga"),
        P(),
        P(),
        P(None, ("band", "ga")),
        P(("band", "ga")),
    )
    out_specs = P(None, "ga", "band", None)
    return jax.shard_map(
        on_device, mesh=mesh, in_specs=in_specs, out_specs=out_specs, check_vma=False
    )
```
